768 devices in a mesh: dp: 96 (over x, z, y_lo), mp: 8 (over y_hi, core).
Axes of the slice: x: 4, y: 8 (y_hi: 4, y_lo: 2; y = y_hi * 2 + y_lo), z: 12, core: 2. Of those that a mesh axis runs over, the one named last changes fastest.
Arguments:
- q_latent: bfloat16 [24576, 2, 768], P('dp', None, 'mp'), may hold values from -6 to 6
- kv_latent: bfloat16 [24576, 2, 256], P('dp', None, 'mp'), may hold values from -6 to 6
- q_head_grad: bfloat16 [24576, 6144], P('dp'), may hold values from -0.125 to 0.125
- k_head_grad: bfloat16 [24576, 6144], P('dp'), may hold values from -0.125 to 0.125
- q_heads: bfloat16 [24576, 6144], P('dp', 'mp'), may hold values from -6 to 6
- k_heads: bfloat16 [24576, 6144], P('dp', 'mp'), may hold values from -6 to 6
- query_pick: int32 [96, 16, 48], P('dp', None, 'mp'), may hold values from 0 to 255
- key_pick: int32 [96, 16, 48], P('dp', None, 'mp'), may hold values from 0 to 255
- q_weight: float32 [96, 768, 128], P('dp', 'mp'), may hold values from -6 to 6
- k_weight: float32 [96, 256, 128], P('dp', 'mp'), may hold values from -6 to 6
- q_moment: float32 [96, 768, 128], P('dp', 'mp'), may hold values from -6 to 6
- k_moment: float32 [96, 256, 128], P('dp', 'mp'), may hold values from -6 to 6
Outputs:
- q_weight_new: float32 [96, 768, 128], P('dp', 'mp')
- k_weight_new: float32 [96, 256, 128], P('dp', 'mp')
- q_moment_new: float32 [96, 768, 128], P('dp', 'mp')
- k_moment_new: float32 [96, 256, 128], P('dp', 'mp')
The draws below stay inside these ranges and needn't reach their ends.
Inputs may be any that keep to these rules, and one draw needn't show every extreme that they name: `query_pick`: the index of a token among the 256 tokens of its own block b. `key_pick`: the index of a token among the 256 tokens of its own block b.
All inputs are finite; a program needn't handle non-finite values.
Results may differ from the reference program's by a relative error of at most 0.0003.
Values sent between devices are 32-bit elements; how exact they have to be, the bound alone decides.
A program may use at most 64 MiB of HBM per device.

```python
import math
import jax
import jax.numpy as jnp
from jax import lax

QR = 1536
KR = 512
DN = 128
TOK_DEV = 256
PICKS = 16
ITERS = 5
HEADS = 48
TOKENS = 24576
N_DP = 96


def touch_ends(result, stream_key, low, top_value):
    dims = result.shape
    spot = [jax.random.randint(jax.random.fold_in(stream_key, axis), (), 0, dims[axis]) for axis in range(len(dims))]
    result = result.at[tuple(spot)].set(low)
    longest = dims.index(max(dims))
    spot[longest] = (spot[longest] + 1) % dims[longest]
    return result.at[tuple(spot)].set(top_value)


def strengthened(result, stream_key, source, target, parts, factor):
    owner, partner = [(jnp.arange(result.shape[axis_at]) // (result.shape[axis_at] // parts)).reshape([-1 if axis == axis_at else 1 for axis in range(result.ndim)]) for axis_at in (source, target)]
    chosen = jax.random.permutation(stream_key, parts)[partner]
    strong = (owner == chosen) | (owner == (partner + parts // 2) % parts)
    return jnp.where(strong, factor * result, result)


def levels(key, dims, pieces, low, high):
    def one(position, shards_of):
        steps = jax.random.uniform(jax.random.fold_in(jax.random.fold_in(key, 6), position), (shards_of,), jnp.float32, low / len(pieces), high / len(pieces))
        return jnp.repeat(jnp.exp(steps), dims[position] // shards_of).reshape((-1,) + (1,) * (len(dims) - position - 1))

    loudness = one(*pieces[0])
    for cut in pieces[1:]:
        loudness = loudness * one(*cut)
    return loudness


def gaussian(own_key, extent, spread, bound, cuts=(), kind=jnp.bfloat16):
    result = spread * jax.random.normal(own_key, extent, jnp.float32)
    if cuts:
        result = result * levels(own_key, extent, cuts, -0.22, 0.18)
    return jnp.clip(result, -bound, bound).astype(kind)


def bell_draw_with(rng, dims, scale, limit, shards, heavy, held_as=jnp.bfloat16):
    entries = scale * jax.random.normal(rng, dims, jnp.float32)
    if shards:
        entries = entries * levels(rng, dims, shards, -0.22, 0.18)
    return jnp.clip(strengthened(entries, jax.random.fold_in(rng, 3), *heavy), -limit, limit).astype(held_as)


def setup_inputs(seed: int = 0) -> dict:
    key_list = jax.random.split(jax.random.key(seed), 13)
    return {
        "q_latent": gaussian(key_list[0], (TOKENS, 2, QR // 2), 1.0, 6.0, ((0, 96), (2, 8))),
        "kv_latent": gaussian(key_list[1], (TOKENS, 2, KR // 2), 1.0, 6.0, ((0, 96), (2, 8))),
        "q_head_grad": bell_draw_with(key_list[2], (TOKENS, HEADS * DN), TOKENS ** -0.5, 0.125, ((0, 96),), (0, 1, 96, 4.75)),
        "k_head_grad": bell_draw_with(key_list[3], (TOKENS, HEADS * DN), TOKENS ** -0.5, 0.125, ((0, 96),), (0, 1, 96, 4.75)),
        "q_heads": gaussian(key_list[4], (TOKENS, HEADS * DN), 1.0, 6.0, ((0, 96), (1, 8))),
        "k_heads": gaussian(key_list[5], (TOKENS, HEADS * DN), 1.0, 6.0, ((0, 96), (1, 8))),
        "query_pick": touch_ends(jax.random.randint(key_list[6], (N_DP, PICKS, HEADS), 0, TOK_DEV), jax.random.fold_in(key_list[6], 1), 0, TOK_DEV - 1).astype(jnp.int32),
        "key_pick": touch_ends(jax.random.randint(key_list[7], (N_DP, PICKS, HEADS), 0, TOK_DEV), jax.random.fold_in(key_list[7], 1), 0, TOK_DEV - 1).astype(jnp.int32),
        "q_weight": gaussian(key_list[8], (2 * HEADS, QR // 2, DN), 1.0, 6.0, ((0, 96), (1, 8)), jnp.float32),
        "k_weight": gaussian(key_list[9], (2 * HEADS, KR // 2, DN), 1.0, 6.0, ((0, 96), (1, 8)), jnp.float32),
        "q_moment": gaussian(key_list[10], (2 * HEADS, QR // 2, DN), 1.0, 6.0, ((0, 96), (1, 8)), jnp.float32),
        "k_moment": gaussian(key_list[11], (2 * HEADS, KR // 2, DN), 1.0, 6.0, ((0, 96), (1, 8)), jnp.float32),
    }


MOMENTUM = 0.95
STEP_SIZE = 1.0
DECAY = 0.1
CLIP_LEVEL = 0.1
SCORE_SCALE = 1.0 / math.sqrt(192.0)
COEFF_A = 3.4445
COEFF_B = -4.775
COEFF_C = 2.0315
HIGHEST = lax.Precision.HIGHEST

def grad_slots(latent, head_grad):
    flat = latent.reshape(latent.shape[0], -1)
    total = jnp.dot(flat.T, head_grad, preferred_element_type=jnp.float32)
    rows_all = total.shape[0]
    total = total.reshape(2, rows_all // 2, HEADS, DN).transpose(0, 2, 1, 3)
    return total.reshape(2 * HEADS, rows_all // 2, DN)

def to_heads(slots):
    count, half_rows, width = slots.shape
    stacked = slots.reshape(2, count // 2, half_rows, width).transpose(1, 0, 2, 3)
    return stacked.reshape(count // 2, 2 * half_rows, width)

def to_slots(stacked):
    heads, rows_all, width = stacked.shape
    split = stacked.reshape(heads, 2, rows_all // 2, width).transpose(1, 0, 2, 3)
    return split.reshape(2 * heads, rows_all // 2, width)

def gramians(stacked):
    return jnp.einsum('hrc,hrd->hcd', stacked, stacked, precision=HIGHEST)

def polar(stacked):
    grams = gramians(stacked)
    scale = 1.0 / jnp.sqrt(jnp.trace(grams, axis1=1, axis2=2) + 1.0)
    current = stacked * scale[:, None, None]
    grams = grams * (scale * scale)[:, None, None]
    for step in range(ITERS):
        square = jnp.einsum('hcd,hde->hce', grams, grams, precision=HIGHEST)
        mixer = COEFF_B * grams + COEFF_C * square
        current = COEFF_A * current + jnp.einsum('hrc,hcd->hrd', current, mixer, precision=HIGHEST)
        if step + 1 < ITERS:
            grams = gramians(current)
    return current

def head_peaks(q_heads, k_heads, query_pick, key_pick):
    q_cube = q_heads.reshape(N_DP, TOK_DEV, HEADS, DN)
    k_cube = k_heads.reshape(N_DP, TOK_DEV, HEADS, DN)
    picked_q = jnp.take_along_axis(q_cube, query_pick.astype(jnp.int32)[..., None], axis=1)
    picked_k = jnp.take_along_axis(k_cube, key_pick.astype(jnp.int32)[..., None], axis=1)
    scores = lax.optimization_barrier(jnp.sum(picked_q.astype(jnp.float32) * picked_k.astype(jnp.float32), axis=3)) * SCORE_SCALE
    return lax.optimization_barrier(jnp.max(scores, axis=(0, 1)))

def reference(q_latent, kv_latent, q_head_grad, k_head_grad, q_heads, k_heads, query_pick, key_pick, q_weight, k_weight, q_moment, k_moment):
    q_moment_new = MOMENTUM * q_moment + grad_slots(q_latent, q_head_grad)
    k_moment_new = MOMENTUM * k_moment + grad_slots(kv_latent, k_head_grad)
    q_ortho = to_slots(polar(to_heads(q_moment_new)))
    k_ortho = to_slots(polar(to_heads(k_moment_new)))
    peak = head_peaks(q_heads, k_heads, query_pick, key_pick)
    shrink = jnp.sqrt(CLIP_LEVEL / jnp.maximum(peak, CLIP_LEVEL))
    shrink_slots = jnp.concatenate([shrink, shrink])[:, None, None]
    keep = 1.0 - STEP_SIZE * DECAY
    q_weight_new = (q_weight * keep - STEP_SIZE * 0.2 * math.sqrt(QR) * q_ortho) * shrink_slots
    k_weight_new = (k_weight * keep - STEP_SIZE * 0.2 * math.sqrt(KR) * k_ortho) * shrink_slots
    return (q_weight_new, k_weight_new, q_moment_new, k_moment_new)
```

```python
import functools
import heapq
import math

import jax
import jax.numpy as jnp
from jax import lax
from jax.experimental import pallas as pl
from jax.experimental.pallas import tpu as pltpu
from jax.sharding import Mesh
from jax.sharding import PartitionSpec as P

QR = 1536
KR = 512
ITERS = 5
AXES = ("dp_0", "dp_1", "dp_2", "mp_0", "mp_1")
DP = AXES[:3]
MP = AXES[3:]
SHAPE = (4, 12, 2, 4, 2)

MOMENTUM = 0.95
STEP_SIZE = 1.0
DECAY = 0.1
CLIP_LEVEL = 0.1
SCORE_SCALE = 1.0 / math.sqrt(192.0)
COEFF_A = 3.4445
COEFF_B = -4.775
COEFF_C = 2.0315
LOWEST = -1e30
W = 128
PEAK_ROWS = 8


def chains(n, parity):
    far, near = n // 2, n - 1 - n // 2
    return {-1: far, 1: near} if parity == 0 else {-1: near, 1: far}


def message_bytes(stream, stage, sizes):
    size = stream["rows"] * W * 4
    if not stream["peak"]:
        for axis in stream["order"][stage + 1 :]:
            size *= sizes[axis]
    return size


def plan(streams, sizes, rate=46.6e3, latency=2.4, backlog=8.0, turn=0.15):
    free, pool, acts, events, left = {}, [], [], [], {}
    count = 0

    def start_stage(i, k):
        stream = streams[i]
        lengths = chains(sizes[stream["order"][k]], stream["parity"])
        left[i, k] = sum(length > 0 for length in lengths.values())
        for way, length in lengths.items():
            if length > 0:
                pool.append(((-k if k else 1, -length if k == 0 else 0, i), (i, k, way, 0)))

    def fill(now):
        nonlocal count
        pool.sort()
        kept = []
        for item in pool:
            i, k, way, _ = item[1]
            axis = streams[i]["order"][k]
            link = (axis, way if sizes[axis] > 2 else 0)
            if free.get(link, 0.0) - now < backlog:
                begin = max(free.get(link, 0.0), now)
                free[link] = begin + message_bytes(streams[i], k, sizes) / rate
                count += 1
                heapq.heappush(events, (free[link] + latency, count, item[1]))
                acts.append(("send",) + item[1])
            else:
                kept.append(item)
        pool[:] = kept

    now = 0.0
    for i in range(len(streams)):
        start_stage(i, 0)
    fill(now)
    while events:
        at, _, (i, k, way, t) = heapq.heappop(events)
        now = max(now, at) + turn
        stream = streams[i]
        length = chains(sizes[stream["order"][k]], stream["parity"])[way]
        acts.append(("recv", i, k, way, t))
        if t < length - 1:
            pool.append(((-k if k else 0, -(length - t), i), (i, k, way, t + 1)))
        else:
            left[i, k] -= 1
            if left[i, k] == 0:
                acts.append(("close", i, k))
                if k < 2:
                    start_stage(i, k + 1)
        fill(now)
    return acts


def make_streams(q_rows, k_rows):
    piece = q_rows // 6
    streams = [dict(peak=True, rows=PEAK_ROWS, order=(0, 2, 1), parity=0)]
    for n in range(4):
        streams.append(
            dict(peak=False, kind=0, at=n * piece, rows=piece, order=(0, 2, 1), parity=n % 2)
        )
    for n in range(4, 6):
        streams.append(
            dict(peak=False, kind=0, at=n * piece, rows=piece, order=(1, 0, 2), parity=n % 2)
        )
    for n in range(2):
        streams.append(
            dict(
                peak=False,
                kind=1,
                at=n * (k_rows // 2),
                rows=k_rows // 2,
                order=(1, 0, 2),
                parity=n % 2,
            )
        )
    return streams


def split(x):
    high = x.astype(jnp.bfloat16)
    low = (x - high.astype(jnp.float32)).astype(jnp.bfloat16)
    return jnp.concatenate([high, low], axis=1)


def contract_rows(a, b):
    return lax.dot_general(a, b, (((0,), (0,)), ((), ())), preferred_element_type=jnp.float32)


def gramian(pair):
    g = contract_rows(pair, pair)
    return (g[:W, :W] + g[W:, W:]) + (g[:W, W:] + g[W:, :W])


def mixer_of(gram):
    square = jnp.dot(
        gram, gram, precision=lax.Precision.HIGHEST, preferred_element_type=jnp.float32
    )
    mixer = split(COEFF_B * gram + COEFF_C * square)
    return jnp.concatenate([mixer, mixer], axis=0)


def mixed(pair, mixer):
    out = jnp.dot(pair, mixer, preferred_element_type=jnp.float32)
    return out[:, :W] + out[:, W:]


def body(
    sizes,
    q_rows,
    k_rows,
    picks,
    tokens,
    local_heads,
    streams,
    acts,
    q_lat,
    k_lat,
    q_grad_hbm,
    k_grad_hbm,
    q_heads,
    k_heads,
    q_pick,
    k_pick,
    q_weight,
    k_weight,
    q_moment,
    k_moment,
    q_weight_out,
    k_weight_out,
    q_moment_out,
    k_moment_out,
    *scratch,
):
    nx, nz, ny, nh, nc = sizes
    q_grad, k_grad, blocks, x_full, pairs, in_sem, send_sem, recv_sem = scratch[:8]
    bufs = scratch[8:]
    me = tuple(lax.axis_index(name) for name in AXES)
    rows = q_rows + k_rows

    def at(axis, shift):
        there = list(me)
        there[axis] = lax.rem(me[axis] + shift + sizes[axis], sizes[axis])
        return tuple(there)

    reads = [
        pltpu.make_async_copy(q_grad_hbm, q_grad, in_sem.at[0]),
        pltpu.make_async_copy(k_grad_hbm, k_grad, in_sem.at[1]),
    ]
    for read in reads:
        read.start()
    partners = []
    for axis in range(3):
        shifts = {1 % sizes[axis], sizes[axis] - 1}
        if axis == 0:
            shifts.add(nx // 2)
        partners += [at(axis, s) for s in sorted(shifts) if s]
    partners += [at(3, s) for s in range(1, nh)] + [at(4, s) for s in range(1, nc)]
    barrier = pltpu.get_barrier_semaphore()
    for there in partners:
        pl.semaphore_signal(
            barrier, inc=1, device_id=there, device_id_type=pl.DeviceIdType.MESH
        )

    place = me[3] * nc + me[4]
    lane = lax.broadcasted_iota(jnp.int32, (PEAK_ROWS, W), 1)
    token = lax.broadcasted_iota(jnp.int32, (tokens, picks), 0)
    peaks = jnp.full((PEAK_ROWS, W), LOWEST, jnp.float32)
    for h in range(local_heads):
        picked = []
        for pick, heads in ((q_pick, q_heads), (k_pick, k_heads)):
            chosen = (token == pick[h : h + 1, :]).astype(jnp.float32).astype(jnp.bfloat16)
            picked.append(contract_rows(chosen, heads[:, h * W : (h + 1) * W]))
        score = jnp.sum(picked[0] * picked[1], axis=1, keepdims=True)
        top = jnp.max(score, axis=0, keepdims=True) * SCORE_SCALE
        peaks = jnp.where(lane == place * local_heads + h, top, peaks)
    bufs[0][...] = peaks
    pl.semaphore_wait(barrier, len(partners))

    shaped, slot_of, sem_of, sems, pos = [], [], {}, 0, 0
    for i, stream in enumerate(streams):
        shaped.append(bufs[pos : pos + 6])
        pos += 6
        slots = {}
        for k in range(3):
            number = 0
            lengths = chains(sizes[stream["order"][k]], stream["parity"])
            for way, length in lengths.items():
                for t in range(length):
                    slots[k, way, t] = number
                    sem_of[i, k, way, t] = sems
                    number += 1
                    sems += 1
        slot_of.append(slots)

    for read in reads:
        read.wait()

    def terms(j, carry):
        x_low, z = j // nz, lax.rem(j, nz)
        cols = pl.ds(pl.multiple_of(j * (ny * W), ny * W), ny * W)
        out = (
            jnp.dot(q_lat[...], q_grad[:, cols], preferred_element_type=jnp.float32),
            jnp.dot(k_lat[...], k_grad[:, cols], preferred_element_type=jnp.float32),
        )
        for stream, buf in zip(streams, shaped):
            if stream["peak"]:
                continue
            for half in range(2):
                first = half * (q_rows, k_rows)[stream["kind"]] + stream["at"]
                for y in range(ny):
                    where = {0: half * (nx // 2) + x_low, 1: z, 2: y}
                    a, b, c = (where[axis] for axis in stream["order"])
                    buf[0][a, b, c] = out[stream["kind"]][
                        first : first + stream["rows"], y * W : (y + 1) * W
                    ]
        return carry

    lax.fori_loop(0, nx // 2 * nz, terms, 0)

    def join(stream, a, b):
        return jnp.maximum(a, b) if stream["peak"] else a + b

    def own_part(i, k, which):
        stream, buf = streams[i], shaped[i]
        source = (buf[0], buf[2], buf[4])[k]
        return source if stream["peak"] else source.at[which]

    def remote(i, k, way, t):
        stream, buf = streams[i], shaped[i]
        axis = stream["order"][k]
        landing = (buf[1], buf[3], buf[5])[k]
        length = chains(sizes[axis], stream["parity"])[way]
        if t == 0:
            which = lax.rem(me[axis] + way * length + sizes[axis], sizes[axis])
            source = own_part(i, k, which)
        else:
            source = landing.at[slot_of[i][k, way, t - 1]]
        sem = sem_of[i, k, way, t]
        return pltpu.make_async_remote_copy(
            src_ref=source,
            dst_ref=landing.at[slot_of[i][k, way, t]],
            send_sem=send_sem.at[sem],
            recv_sem=recv_sem.at[sem],
            device_id=at(axis, way),
            device_id_type=pl.DeviceIdType.MESH,
        )

    half = me[0] // (nx // 2)
    mine = blocks.at[half, me[3], me[4]]
    started = []
    for act in acts:
        if act[0] == "send":
            copy = remote(*act[1:])
            copy.start()
            started.append(copy)
        elif act[0] == "recv":
            _, i, k, way, t = act
            remote(i, k, way, t).wait_recv()
            stream = streams[i]
            axis = stream["order"][k]
            length = chains(sizes[axis], stream["parity"])[way]
            if t < length - 1:
                landed = (shaped[i][1], shaped[i][3], shaped[i][5])[k].at[slot_of[i][k, way, t]]
                which = lax.rem(me[axis] + way * (length - t - 1) + sizes[axis], sizes[axis])
                landed[...] = join(stream, landed[...], own_part(i, k, which)[...])
        else:
            _, i, k = act
            stream = streams[i]
            axis = stream["order"][k]
            total = own_part(i, k, me[axis])[...]
            landing = (shaped[i][1], shaped[i][3], shaped[i][5])[k]
            for way, length in chains(sizes[axis], stream["parity"]).items():
                if length > 0:
                    total = join(stream, total, landing[slot_of[i][k, way, length - 1]])
            if k < 2:
                (shaped[i][2], shaped[i][4])[k][...] = total
            elif stream["peak"]:
                mine[rows:, :] = total
            else:
                span = pl.ds(stream["at"], stream["rows"])
                moment, out = ((q_moment, q_moment_out), (k_moment, k_moment_out))[stream["kind"]]
                fresh = MOMENTUM * moment[span, :] + total
                out[span, :] = fresh
                mine[pl.ds(stream["kind"] * q_rows + stream["at"], stream["rows"]), :] = fresh

    gathered = sems
    sent = 0

    def hand_on(which, there):
        nonlocal sent
        h, y, c = which
        number = (h * nh + y) * nc + c
        copy = pltpu.make_async_remote_copy(
            src_ref=blocks.at[h, y, c],
            dst_ref=blocks.at[h, y, c],
            send_sem=send_sem.at[gathered + sent],
            recv_sem=recv_sem.at[gathered + number],
            device_id=there,
            device_id_type=pl.DeviceIdType.MESH,
        )
        copy.start()
        started.append(copy)
        sent += 1

    def arrived(which):
        h, y, c = which
        number = (h * nh + y) * nc + c
        pltpu.make_async_remote_copy(
            src_ref=blocks.at[h, y, c],
            dst_ref=blocks.at[h, y, c],
            send_sem=send_sem.at[gathered],
            recv_sem=recv_sem.at[gathered + number],
            device_id=me,
            device_id_type=pl.DeviceIdType.MESH,
        ).wait_recv()

    own = (half, me[3], me[4])
    far = (1 - half, me[3], me[4])
    hand_on(own, at(0, nx // 2))
    for s in range(1, nh):
        hand_on(own, at(3, s))
    for s in range(1, nc):
        hand_on(own, at(4, s))
    arrived(far)
    for s in range(1, nh):
        hand_on(far, at(3, s))
    for s in range(1, nc):
        hand_on(far, at(4, s))
    for h in (half, 1 - half):
        for s in range(1, nh):
            other = (h, lax.rem(me[3] - s + nh, nh), me[4])
            arrived(other)
            for s2 in range(1, nc):
                hand_on(other, at(4, s2))
    for s2 in range(1, nc):
        for h in (half, 1 - half):
            for s in range(nh):
                arrived((h, lax.rem(me[3] - s + nh, nh), lax.rem(me[4] - s2 + nc, nc)))
    for copy in started:
        copy.wait_send()

    head = lax.rem((me[0] * nz + me[1]) * ny + me[2], nx * nz * ny // 2)
    top = jnp.full((PEAK_ROWS, W), LOWEST, jnp.float32)
    for y in range(nh):
        for c in range(nc):
            top = jnp.maximum(top, blocks[half, y, c, rows:, :])
    top = jnp.where(lane == head, top, LOWEST)
    peak = jnp.max(jnp.max(top, axis=1, keepdims=True), axis=0, keepdims=True)
    shrink = jnp.sqrt(CLIP_LEVEL / jnp.maximum(peak, CLIP_LEVEL))

    count = 2 * nh * nc
    starts = (0, count * q_rows)
    heights = (count * q_rows, count * k_rows)
    for h in range(2):
        for y in range(nh):
            for c in range(nc):
                number = (h * nh + y) * nc + c
                block = blocks[h, y, c]
                for kind, part in ((0, block[:q_rows]), (1, block[q_rows:rows])):
                    height = (q_rows, k_rows)[kind]
                    span = pl.ds(starts[kind] + number * height, height)
                    x_full[span, :] = part
                    pairs[span, :] = split(part)

    def tile(kind):
        return pl.ds(starts[kind], heights[kind])

    eye = lax.broadcasted_iota(jnp.int32, (W, W), 0) == lax.broadcasted_iota(
        jnp.int32, (W, W), 1
    )
    mixers, scales = [], []
    for kind in range(2):
        gram = gramian(pairs[tile(kind), :])
        diagonal = jnp.where(eye, gram, 0.0)
        trace = jnp.sum(jnp.sum(diagonal, axis=1, keepdims=True), axis=0, keepdims=True)
        scale = 1.0 / jnp.sqrt(trace + 1.0)
        mixers.append(mixer_of(gram * (scale * scale)))
        scales.append(scale)
    for kind in range(2):
        fresh = scales[kind] * (
            COEFF_A * x_full[tile(kind), :] + mixed(pairs[tile(kind), :], mixers[kind])
        )
        x_full[tile(kind), :] = fresh
        pairs[tile(kind), :] = split(fresh)

    def iteration(_, carry):
        mixers = [mixer_of(gramian(pairs[tile(kind), :])) for kind in range(2)]
        for kind in range(2):
            fresh = COEFF_A * x_full[tile(kind), :] + mixed(pairs[tile(kind), :], mixers[kind])
            x_full[tile(kind), :] = fresh
            pairs[tile(kind), :] = split(fresh)
        return carry

    lax.fori_loop(0, ITERS - 2, iteration, 0)
    number = (half * nh + me[3]) * nc + me[4]
    keep = 1.0 - STEP_SIZE * DECAY
    for kind, (weight, out, rank) in enumerate(
        ((q_weight, q_weight_out, QR), (k_weight, k_weight_out, KR))
    ):
        height = (q_rows, k_rows)[kind]
        mixer = mixer_of(gramian(pairs[tile(kind), :]))
        span = pl.ds(pl.multiple_of(starts[kind] + number * height, 8), height)
        current = x_full[span, :]
        ortho = COEFF_A * current + mixed(split(current), mixer)
        out[...] = (weight[...] * keep - STEP_SIZE * 0.2 * math.sqrt(rank) * ortho) * shrink


def step(sizes, q_rows, k_rows, picks, tokens, local_heads):
    streams = make_streams(q_rows, k_rows)
    acts = plan(streams, sizes)
    rows = q_rows + k_rows
    width = sizes[0] * sizes[1] * sizes[2] // 2 * W
    count = 2 * sizes[3] * sizes[4]
    scratch = [
        pltpu.VMEM((tokens, width), jnp.bfloat16),
        pltpu.VMEM((tokens, width), jnp.bfloat16),
        pltpu.VMEM((2, sizes[3], sizes[4], rows + PEAK_ROWS, W), jnp.float32),
        pltpu.VMEM((count * rows, W), jnp.float32),
        pltpu.VMEM((count * rows, 2 * W), jnp.bfloat16),
        pltpu.SemaphoreType.DMA((2,)),
    ]
    messages = 0
    bufs = []
    for stream in streams:
        n = [sizes[axis] for axis in stream["order"]]
        messages += sum(n) - 3
        tile = (stream["rows"], W)
        lead = [(), (), ()] if stream["peak"] else [(n[1], n[2]), (n[2],), ()]
        for k in range(3):
            source = lead[k] if stream["peak"] else (n[k],) + lead[k]
            bufs.append(pltpu.VMEM(source + tile, jnp.float32))
            bufs.append(pltpu.VMEM((max(n[k] - 1, 1),) + lead[k] + tile, jnp.float32))
    scratch += [
        pltpu.SemaphoreType.DMA((messages + count,)),
        pltpu.SemaphoreType.DMA((messages + count,)),
    ]
    vmem = pl.BlockSpec(memory_space=pltpu.VMEM)
    hbm = pl.BlockSpec(memory_space=pl.ANY)
    return pl.pallas_call(
        functools.partial(
            body, sizes, q_rows, k_rows, picks, tokens, local_heads, streams, acts
        ),
        out_shape=[
            jax.ShapeDtypeStruct((q_rows, W), jnp.float32),
            jax.ShapeDtypeStruct((k_rows, W), jnp.float32),
            jax.ShapeDtypeStruct((q_rows, W), jnp.float32),
            jax.ShapeDtypeStruct((k_rows, W), jnp.float32),
        ],
        in_specs=[vmem, vmem, hbm, hbm] + [vmem] * 8,
        out_specs=[vmem] * 4,
        scratch_shapes=scratch + bufs,
        compiler_params=pltpu.CompilerParams(
            collective_id=0, has_side_effects=True, vmem_limit_bytes=60 * 1024 * 1024
        ),
        name="muon_clip",
    )


def local(
    sizes,
    q_latent,
    kv_latent,
    q_head_grad,
    k_head_grad,
    q_heads,
    k_heads,
    query_pick,
    key_pick,
    q_weight,
    k_weight,
    q_moment,
    k_moment,
):
    tokens, _, q_rows = q_latent.shape
    k_rows = kv_latent.shape[2]
    picks, local_heads = query_pick.shape[1:]
    out = step(sizes, q_rows, k_rows, picks, tokens, local_heads)(
        q_latent.transpose(1, 2, 0).reshape(2 * q_rows, tokens),
        kv_latent.transpose(1, 2, 0).reshape(2 * k_rows, tokens),
        q_head_grad,
        k_head_grad,
        q_heads,
        k_heads,
        query_pick[0].T,
        key_pick[0].T,
        q_weight[0],
        k_weight[0],
        q_moment[0],
        k_moment[0],
    )
    return tuple(array[None] for array in out)


def solution(mesh, sizes=SHAPE):
    axes = Mesh(mesh.devices.reshape(sizes), AXES)
    placed = (
        P(DP, None, MP),
        P(DP, None, MP),
        P(DP, None),
        P(DP, None),
        P(DP, MP),
        P(DP, MP),
        P(DP, None, MP),
        P(DP, None, MP),
        P(DP, MP, None),
        P(DP, MP, None),
        P(DP, MP, None),
        P(DP, MP, None),
    )
    return jax.shard_map(
        functools.partial(local, sizes),
        mesh=axes,
        in_specs=placed,
        out_specs=(P(DP, MP, None),) * 4,
        check_vma=False,
    )
```

```python
import functools
import heapq
import math

import jax
import jax.numpy as jnp
from jax import lax
from jax.experimental import pallas as pl
from jax.experimental.pallas import tpu as pltpu
from jax.sharding import Mesh
from jax.sharding import PartitionSpec as P

QR = 1536
KR = 512
ITERS = 5
AXES = ("dp_0", "dp_1", "dp_2", "mp_0", "mp_1")
DP = AXES[:3]
MP = AXES[3:]
SHAPE = (4, 12, 2, 4, 2)

MOMENTUM = 0.95
STEP_SIZE = 1.0
DECAY = 0.1
CLIP_LEVEL = 0.1
SCORE_SCALE = 1.0 / math.sqrt(192.0)
COEFF_A = 3.4445
COEFF_B = -4.775
COEFF_C = 2.0315
LOWEST = -1e30
W = 128
PEAK_ROWS = 8


def chains(n, parity):
    far, near = n // 2, n - 1 - n // 2
    return {-1: far, 1: near} if parity == 0 else {-1: near, 1: far}


def message_bytes(stream, stage, sizes):
    size = stream["rows"] * W * 4
    if not stream["peak"]:
        for axis in stream["order"][stage + 1 :]:
            size *= sizes[axis]
    return size


def plan(streams, sizes, rate=46.6e3, latency=2.4, backlog=8.0, turn=0.15, rest=3.5):
    free, pool, acts, events, left = {}, [], [], [], {}
    count = 0

    def start_stage(i, k):
        stream = streams[i]
        lengths = chains(sizes[stream["order"][k]], stream["parity"])
        left[i, k] = sum(length > 0 for length in lengths.values())
        for way, length in lengths.items():
            if length > 0:
                pool.append(((-k if k else 1, -length if k == 0 else 0, i), (i, k, way, 0)))

    def fill(now):
        nonlocal count
        pool.sort()
        kept = []
        for item in pool:
            i, k, way, _ = item[1]
            axis = streams[i]["order"][k]
            link = (axis, way if sizes[axis] > 2 else 0)
            if free.get(link, 0.0) - now < backlog:
                begin = max(free.get(link, 0.0), now)
                free[link] = begin + message_bytes(streams[i], k, sizes) / rate
                count += 1
                heapq.heappush(events, (free[link] + latency, count, item[1]))
                acts.append(("send",) + item[1])
            else:
                kept.append(item)
        pool[:] = kept

    early = [i for i, stream in enumerate(streams) if stream["order"][0] == 1]
    now = 0.0
    for i in early:
        start_stage(i, 0)
    fill(now)
    acts.append(("rest",))
    now = rest
    for i in range(len(streams)):
        if i not in early:
            start_stage(i, 0)
    fill(now)
    while events:
        at, _, (i, k, way, t) = heapq.heappop(events)
        now = max(now, at) + turn
        stream = streams[i]
        length = chains(sizes[stream["order"][k]], stream["parity"])[way]
        acts.append(("recv", i, k, way, t))
        if t < length - 1:
            pool.append(((-k if k else 0, -(length - t), i), (i, k, way, t + 1)))
        else:
            left[i, k] -= 1
            if left[i, k] == 0:
                acts.append(("close", i, k))
                if k < 2:
                    start_stage(i, k + 1)
        fill(now)
    return acts


def make_streams(q_rows, k_rows):
    piece = q_rows // 6
    streams = [dict(peak=True, rows=PEAK_ROWS, order=(0, 2, 1), parity=0)]
    for n in range(4):
        streams.append(
            dict(peak=False, kind=0, at=n * piece, rows=piece, order=(0, 2, 1), parity=n % 2)
        )
    for n in range(4, 6):
        streams.append(
            dict(peak=False, kind=0, at=n * piece, rows=piece, order=(1, 0, 2), parity=n % 2)
        )
    for n in range(2):
        streams.append(
            dict(
                peak=False,
                kind=1,
                at=n * (k_rows // 2),
                rows=k_rows // 2,
                order=(1, 0, 2),
                parity=n % 2,
            )
        )
    return streams


def split(x):
    high = x.astype(jnp.bfloat16)
    low = (x - high.astype(jnp.float32)).astype(jnp.bfloat16)
    return jnp.concatenate([high, low], axis=1)


def contract_rows(a, b):
    return lax.dot_general(a, b, (((0,), (0,)), ((), ())), preferred_element_type=jnp.float32)


def gramian(pair):
    g = contract_rows(pair, pair)
    return (g[:W, :W] + g[W:, W:]) + (g[:W, W:] + g[W:, :W])


def mixer_of(gram):
    square = jnp.dot(
        gram, gram, precision=lax.Precision.HIGHEST, preferred_element_type=jnp.float32
    )
    mixer = split(COEFF_B * gram + COEFF_C * square)
    return jnp.concatenate([mixer, mixer], axis=0)


def mixed(pair, mixer):
    out = jnp.dot(pair, mixer, preferred_element_type=jnp.float32)
    return out[:, :W] + out[:, W:]


def body(
    sizes,
    q_rows,
    k_rows,
    picks,
    tokens,
    local_heads,
    streams,
    acts,
    q_lat,
    k_lat,
    q_grad_hbm,
    k_grad_hbm,
    q_heads,
    k_heads,
    q_pick,
    k_pick,
    q_weight,
    k_weight,
    q_moment,
    k_moment,
    q_weight_out,
    k_weight_out,
    q_moment_out,
    k_moment_out,
    *scratch,
):
    nx, nz, ny, nh, nc = sizes
    q_grad, k_grad, blocks, x_full, pairs, in_sem, send_sem, recv_sem = scratch[:8]
    bufs = scratch[8:]
    me = tuple(lax.axis_index(name) for name in AXES)
    rows = q_rows + k_rows

    def at(axis, shift):
        there = list(me)
        there[axis] = lax.rem(me[axis] + shift + sizes[axis], sizes[axis])
        return tuple(there)

    def nth_z(n):
        size = nz // 2 - (n + 1) // 2
        return lax.rem(me[1] + (size if n % 2 else -size) + nz, nz)

    def loop_z(n):
        size = nz // 2 - (n + 1) // 2
        return lax.rem(me[1] + jnp.where(lax.rem(n, 2) == 1, size, -size) + nz, nz)

    def reads(n, z):
        copies = []
        for x_low in range(nx // 2):
            cols = pl.ds(pl.multiple_of((x_low * nz + z) * (ny * W), ny * W), ny * W)
            for kind, (source, target) in enumerate(((q_grad_hbm, q_grad), (k_grad_hbm, k_grad))):
                copies.append(
                    pltpu.make_async_copy(
                        source.at[:, cols], target.at[:, cols], in_sem.at[n, x_low, kind]
                    )
                )
        return copies

    for n in range(nz):
        for copy in reads(n, nth_z(n)):
            copy.start()
    partners = []
    for axis in range(3):
        shifts = {1 % sizes[axis], sizes[axis] - 1}
        if axis == 0:
            shifts.add(nx // 2)
        partners += [at(axis, s) for s in sorted(shifts) if s]
    partners += [at(3, s) for s in range(1, nh)] + [at(4, s) for s in range(1, nc)]
    barrier = pltpu.get_barrier_semaphore()
    for there in partners:
        pl.semaphore_signal(
            barrier, inc=1, device_id=there, device_id_type=pl.DeviceIdType.MESH
        )

    place = me[3] * nc + me[4]
    lane = lax.broadcasted_iota(jnp.int32, (PEAK_ROWS, W), 1)
    token = lax.broadcasted_iota(jnp.int32, (tokens, picks), 0)
    peaks = jnp.full((PEAK_ROWS, W), LOWEST, jnp.float32)
    for h in range(local_heads):
        picked = []
        for pick, heads in ((q_pick, q_heads), (k_pick, k_heads)):
            chosen = (token == pick[h]).astype(jnp.float32).astype(jnp.bfloat16)
            picked.append(contract_rows(chosen, heads[:, h * W : (h + 1) * W]))
        score = jnp.sum(picked[0] * picked[1], axis=1, keepdims=True)
        top = jnp.max(score, axis=0, keepdims=True) * SCORE_SCALE
        peaks = jnp.where(lane == place * local_heads + h, top, peaks)
    bufs[0][...] = peaks

    shaped, slot_of, sem_of, sems, pos = [], [], {}, 0, 0
    for i, stream in enumerate(streams):
        shaped.append(bufs[pos : pos + 6])
        pos += 6
        slots = {}
        for k in range(3):
            number = 0
            lengths = chains(sizes[stream["order"][k]], stream["parity"])
            for way, length in lengths.items():
                for t in range(length):
                    slots[k, way, t] = number
                    sem_of[i, k, way, t] = sems
                    number += 1
                    sems += 1
        slot_of.append(slots)

    def terms(n, z):
        for copy in reads(n, z):
            copy.wait()
        for x_low in range(nx // 2):
            cols = pl.ds(pl.multiple_of((x_low * nz + z) * (ny * W), ny * W), ny * W)
            out = (
                jnp.dot(q_lat[...], q_grad[:, cols], preferred_element_type=jnp.float32),
                jnp.dot(k_lat[...], k_grad[:, cols], preferred_element_type=jnp.float32),
            )
            for stream, buf in zip(streams, shaped):
                if stream["peak"]:
                    continue
                for half in range(2):
                    first = half * (q_rows, k_rows)[stream["kind"]] + stream["at"]
                    for y in range(ny):
                        where = {0: half * (nx // 2) + x_low, 1: z, 2: y}
                        a, b, c = (where[axis] for axis in stream["order"])
                        buf[0][a, b, c] = out[stream["kind"]][
                            first : first + stream["rows"], y * W : (y + 1) * W
                        ]

    lead = min(3, nz)
    for n in range(lead):
        terms(n, nth_z(n))
    pl.semaphore_wait(barrier, len(partners))

    def rest_of_terms():
        group = 3 if (nz - lead) % 3 == 0 else 1

        def some(m, carry):
            for g in range(group):
                n = lead + m * group + g
                terms(n, loop_z(n))
            return carry

        lax.fori_loop(0, (nz - lead) // group, some, 0)

    def join(stream, a, b):
        return jnp.maximum(a, b) if stream["peak"] else a + b

    def own_part(i, k, which):
        stream, buf = streams[i], shaped[i]
        source = (buf[0], buf[2], buf[4])[k]
        return source if stream["peak"] else source.at[which]

    def remote(i, k, way, t):
        stream, buf = streams[i], shaped[i]
        axis = stream["order"][k]
        landing = (buf[1], buf[3], buf[5])[k]
        length = chains(sizes[axis], stream["parity"])[way]
        if t == 0:
            which = lax.rem(me[axis] + way * length + sizes[axis], sizes[axis])
            source = own_part(i, k, which)
        else:
            source = landing.at[slot_of[i][k, way, t - 1]]
        sem = sem_of[i, k, way, t]
        return pltpu.make_async_remote_copy(
            src_ref=source,
            dst_ref=landing.at[slot_of[i][k, way, t]],
            send_sem=send_sem.at[sem],
            recv_sem=recv_sem.at[sem],
            device_id=at(axis, way),
            device_id_type=pl.DeviceIdType.MESH,
        )

    half = me[0] // (nx // 2)
    mine = blocks.at[half, me[3], me[4]]
    started = []
    for act in acts:
        if act[0] == "rest":
            rest_of_terms()
        elif act[0] == "send":
            copy = remote(*act[1:])
            copy.start()
            started.append(copy)
        elif act[0] == "recv":
            _, i, k, way, t = act
            remote(i, k, way, t).wait_recv()
            stream = streams[i]
            axis = stream["order"][k]
            length = chains(sizes[axis], stream["parity"])[way]
            if t < length - 1:
                landed = (shaped[i][1], shaped[i][3], shaped[i][5])[k].at[slot_of[i][k, way, t]]
                which = lax.rem(me[axis] + way * (length - t - 1) + sizes[axis], sizes[axis])
                landed[...] = join(stream, landed[...], own_part(i, k, which)[...])
        else:
            _, i, k = act
            stream = streams[i]
            axis = stream["order"][k]
            total = own_part(i, k, me[axis])[...]
            landing = (shaped[i][1], shaped[i][3], shaped[i][5])[k]
            for way, length in chains(sizes[axis], stream["parity"]).items():
                if length > 0:
                    total = join(stream, total, landing[slot_of[i][k, way, length - 1]])
            if k < 2:
                (shaped[i][2], shaped[i][4])[k][...] = total
            elif stream["peak"]:
                mine[rows:, :] = total
            else:
                span = pl.ds(stream["at"], stream["rows"])
                moment, out = ((q_moment, q_moment_out), (k_moment, k_moment_out))[stream["kind"]]
                fresh = MOMENTUM * moment[span, :] + total
                out[span, :] = fresh
                mine[pl.ds(stream["kind"] * q_rows + stream["at"], stream["rows"]), :] = fresh

    gathered = sems
    sent = 0

    def hand_on(which, there):
        nonlocal sent
        h, y, c = which
        number = (h * nh + y) * nc + c
        copy = pltpu.make_async_remote_copy(
            src_ref=blocks.at[h, y, c],
            dst_ref=blocks.at[h, y, c],
            send_sem=send_sem.at[gathered + sent],
            recv_sem=recv_sem.at[gathered + number],
            device_id=there,
            device_id_type=pl.DeviceIdType.MESH,
        )
        copy.start()
        started.append(copy)
        sent += 1

    def arrived(which):
        h, y, c = which
        number = (h * nh + y) * nc + c
        pltpu.make_async_remote_copy(
            src_ref=blocks.at[h, y, c],
            dst_ref=blocks.at[h, y, c],
            send_sem=send_sem.at[gathered],
            recv_sem=recv_sem.at[gathered + number],
            device_id=me,
            device_id_type=pl.DeviceIdType.MESH,
        ).wait_recv()

    own = (half, me[3], me[4])
    far = (1 - half, me[3], me[4])
    hand_on(own, at(0, nx // 2))
    for s in range(1, nh):
        hand_on(own, at(3, s))
    for s in range(1, nc):
        hand_on(own, at(4, s))
    arrived(far)
    for s in range(1, nh):
        hand_on(far, at(3, s))
    for s in range(1, nc):
        hand_on(far, at(4, s))
    for h in (half, 1 - half):
        for s in range(1, nh):
            other = (h, lax.rem(me[3] - s + nh, nh), me[4])
            arrived(other)
            for s2 in range(1, nc):
                hand_on(other, at(4, s2))
    for s2 in range(1, nc):
        for h in (half, 1 - half):
            for s in range(nh):
                arrived((h, lax.rem(me[3] - s + nh, nh), lax.rem(me[4] - s2 + nc, nc)))

    head = lax.rem((me[0] * nz + me[1]) * ny + me[2], nx * nz * ny // 2)
    top = jnp.full((PEAK_ROWS, W), LOWEST, jnp.float32)
    for y in range(nh):
        for c in range(nc):
            top = jnp.maximum(top, blocks[half, y, c, rows:, :])
    top = jnp.where(lane == head, top, LOWEST)
    peak = jnp.max(jnp.max(top, axis=1, keepdims=True), axis=0, keepdims=True)
    shrink = jnp.sqrt(CLIP_LEVEL / jnp.maximum(peak, CLIP_LEVEL))

    count = 2 * nh * nc
    starts = (0, count * q_rows)
    heights = (count * q_rows, count * k_rows)
    for h in range(2):
        for y in range(nh):
            for c in range(nc):
                number = (h * nh + y) * nc + c
                block = blocks[h, y, c]
                for kind, part in ((0, block[:q_rows]), (1, block[q_rows:rows])):
                    height = (q_rows, k_rows)[kind]
                    span = pl.ds(starts[kind] + number * height, height)
                    x_full[span, :] = part
                    pairs[span, :] = split(part)

    def tile(kind):
        return pl.ds(starts[kind], heights[kind])

    eye = lax.broadcasted_iota(jnp.int32, (W, W), 0) == lax.broadcasted_iota(
        jnp.int32, (W, W), 1
    )
    mixers, scales = [], []
    for kind in range(2):
        gram = gramian(pairs[tile(kind), :])
        diagonal = jnp.where(eye, gram, 0.0)
        trace = jnp.sum(jnp.sum(diagonal, axis=1, keepdims=True), axis=0, keepdims=True)
        scale = 1.0 / jnp.sqrt(trace + 1.0)
        mixers.append(mixer_of(gram * (scale * scale)))
        scales.append(scale)
    for kind in range(2):
        fresh = scales[kind] * (
            COEFF_A * x_full[tile(kind), :] + mixed(pairs[tile(kind), :], mixers[kind])
        )
        x_full[tile(kind), :] = fresh
        pairs[tile(kind), :] = split(fresh)

    def iteration(_, carry):
        mixers = [mixer_of(gramian(pairs[tile(kind), :])) for kind in range(2)]
        for kind in range(2):
            fresh = COEFF_A * x_full[tile(kind), :] + mixed(pairs[tile(kind), :], mixers[kind])
            x_full[tile(kind), :] = fresh
            pairs[tile(kind), :] = split(fresh)
        return carry

    lax.fori_loop(0, ITERS - 2, iteration, 0)
    number = (half * nh + me[3]) * nc + me[4]
    keep = 1.0 - STEP_SIZE * DECAY
    for kind, (weight, out, rank) in enumerate(
        ((q_weight, q_weight_out, QR), (k_weight, k_weight_out, KR))
    ):
        height = (q_rows, k_rows)[kind]
        mixer = mixer_of(gramian(pairs[tile(kind), :]))
        span = pl.ds(pl.multiple_of(starts[kind] + number * height, 8), height)
        current = x_full[span, :]
        ortho = COEFF_A * current + mixed(split(current), mixer)
        out[...] = (weight[...] * keep - STEP_SIZE * 0.2 * math.sqrt(rank) * ortho) * shrink
    for copy in started:
        copy.wait_send()


def step(sizes, q_rows, k_rows, picks, tokens, local_heads):
    streams = make_streams(q_rows, k_rows)
    acts = plan(streams, sizes)
    rows = q_rows + k_rows
    width = sizes[0] * sizes[1] * sizes[2] // 2 * W
    count = 2 * sizes[3] * sizes[4]
    scratch = [
        pltpu.VMEM((tokens, width), jnp.bfloat16),
        pltpu.VMEM((tokens, width), jnp.bfloat16),
        pltpu.VMEM((2, sizes[3], sizes[4], rows + PEAK_ROWS, W), jnp.float32),
        pltpu.VMEM((count * rows, W), jnp.float32),
        pltpu.VMEM((count * rows, 2 * W), jnp.bfloat16),
        pltpu.SemaphoreType.DMA((sizes[1], sizes[0] // 2, 2)),
    ]
    messages = 0
    bufs = []
    for stream in streams:
        n = [sizes[axis] for axis in stream["order"]]
        messages += sum(n) - 3
        tile = (stream["rows"], W)
        lead = [(), (), ()] if stream["peak"] else [(n[1], n[2]), (n[2],), ()]
        for k in range(3):
            source = lead[k] if stream["peak"] else (n[k],) + lead[k]
            bufs.append(pltpu.VMEM(source + tile, jnp.float32))
            bufs.append(pltpu.VMEM((max(n[k] - 1, 1),) + lead[k] + tile, jnp.float32))
    scratch += [
        pltpu.SemaphoreType.DMA((messages + count,)),
        pltpu.SemaphoreType.DMA((messages + count,)),
    ]
    vmem = pl.BlockSpec(memory_space=pltpu.VMEM)
    hbm = pl.BlockSpec(memory_space=pltpu.HBM)
    return pl.pallas_call(
        functools.partial(
            body, sizes, q_rows, k_rows, picks, tokens, local_heads, streams, acts
        ),
        out_shape=[
            pltpu.VMEM((q_rows, W), jnp.float32),
            pltpu.VMEM((k_rows, W), jnp.float32),
            pltpu.VMEM((q_rows, W), jnp.float32),
            pltpu.VMEM((k_rows, W), jnp.float32),
        ],
        in_specs=[vmem, vmem, hbm, hbm] + [vmem] * 8,
        out_specs=[vmem] * 4,
        scratch_shapes=scratch + bufs,
        compiler_params=pltpu.CompilerParams(
            collective_id=0, has_side_effects=True, vmem_limit_bytes=60 * 1024 * 1024
        ),
        name="muon_clip",
    )


def hand_out(*refs):
    for source, target in zip(refs[:4], refs[4:]):
        target[...] = source[...]


def handed_out(arrays):
    vmem = pl.BlockSpec(memory_space=pltpu.VMEM)
    return pl.pallas_call(
        hand_out,
        out_shape=[jax.ShapeDtypeStruct(a.shape, a.dtype) for a in arrays],
        in_specs=[vmem] * 4,
        out_specs=[vmem] * 4,
        compiler_params=pltpu.CompilerParams(vmem_limit_bytes=2 * 1024 * 1024),
        name="hand_out",
    )(*arrays)


def local(
    sizes,
    q_latent,
    kv_latent,
    q_head_grad,
    k_head_grad,
    q_heads,
    k_heads,
    query_pick,
    key_pick,
    q_weight,
    k_weight,
    q_moment,
    k_moment,
):
    tokens, _, q_rows = q_latent.shape
    k_rows = kv_latent.shape[2]
    picks, local_heads = query_pick.shape[1:]
    out = step(sizes, q_rows, k_rows, picks, tokens, local_heads)(
        q_latent.transpose(1, 2, 0).reshape(2 * q_rows, tokens),
        kv_latent.transpose(1, 2, 0).reshape(2 * k_rows, tokens),
        q_head_grad,
        k_head_grad,
        q_heads,
        k_heads,
        query_pick.transpose(2, 0, 1),
        key_pick.transpose(2, 0, 1),
        q_weight[0],
        k_weight[0],
        q_moment[0],
        k_moment[0],
    )
    return tuple(array[None] for array in handed_out(out))


def solution(mesh, sizes=SHAPE):
    axes = Mesh(mesh.devices.reshape(sizes), AXES)
    placed = (
        P(DP, None, MP),
        P(DP, None, MP),
        P(DP, None),
        P(DP, None),
        P(DP, MP),
        P(DP, MP),
        P(DP, None, MP),
        P(DP, None, MP),
        P(DP, MP, None),
        P(DP, MP, None),
        P(DP, MP, None),
        P(DP, MP, None),
    )
    return jax.shard_map(
        functools.partial(local, sizes),
        mesh=axes,
        in_specs=placed,
        out_specs=(P(DP, MP, None),) * 4,
        check_vma=False,
    )
```

```python
import functools
import heapq
import math

import jax
import jax.numpy as jnp
from jax import lax
from jax.experimental import pallas as pl
from jax.experimental.pallas import tpu as pltpu
from jax.sharding import Mesh
from jax.sharding import PartitionSpec as P

QR = 1536
KR = 512
ITERS = 5
AXES = ("dp_0", "dp_1", "dp_2", "mp_0", "mp_1")
DP = AXES[:3]
MP = AXES[3:]
SHAPE = (4, 12, 2, 4, 2)

MOMENTUM = 0.95
STEP_SIZE = 1.0
DECAY = 0.1
CLIP_LEVEL = 0.1
SCORE_SCALE = 1.0 / math.sqrt(192.0)
COEFF_A = 3.4445
COEFF_B = -4.775
COEFF_C = 2.0315
LOWEST = -1e30
W = 128
PEAK_ROWS = 8


TREES = {
    2: ((2, 0), (1, 0)),
    3: ((1, 0), (3, 2), (2, 0)),
    5: ((1, 0), (3, 2), (5, 4), (4, 2), (2, 0)),
    6: ((1, 0), (3, 2), (5, 4), (6, 4), (4, 2), (2, 0)),
}


def routes(n, parity, short):
    far, near = n // 2, n - 1 - n // 2
    lengths = {-1: far, 1: near} if parity == 0 else {-1: near, 1: far}
    found = {}
    for way, length in lengths.items():
        if length:
            chain = tuple((f, f - 1) for f in range(length, 0, -1))
            found[way] = TREES.get(length, chain) if short else chain
    return found


def stage_routes(stream, stage, sizes):
    return routes(sizes[stream["order"][stage]], stream["parity"], stream["short"][stage])


def message_bytes(stream, stage, sizes):
    size = stream["rows"] * W * 4
    if not stream["peak"]:
        for axis in stream["order"][stage + 1 :]:
            size *= sizes[axis]
    return size


def plan(streams, sizes, rate=47.5e3, latency=2.5, hop=0.75, backlog=5.0, turn=0.12, rest=3.5):
    free, pool, acts, events, left, missing = {}, [], [], [], {}, {}
    count = 0
    ways = [[stage_routes(stream, k, sizes) for k in range(3)] for stream in streams]

    def sent_to(i, k, way, f):
        return dict(ways[i][k][way])[f]

    def lasts(i, k, way, f):
        time = 0.0
        while f > 0:
            g = sent_to(i, k, way, f)
            time += latency + turn + (f - g - 1) * hop
            time += (f - g) * message_bytes(streams[i], k, sizes) / rate
            f = g
        return time

    def add(i, k, way, f):
        time = lasts(i, k, way, f)
        for later in range(k + 1, 3):
            time += max(
                lasts(i, later, w, start) for w, pairs in ways[i][later].items() for start, _ in pairs
            )
        pool.append((i - time + streams[i]["offset"], (i, k, way, f)))

    def start_stage(i, k):
        left[i, k] = 0
        for way, pairs in ways[i][k].items():
            for f, _ in pairs:
                missing[i, k, way, f] = sum(g == f for _, g in pairs)
                if missing[i, k, way, f] == 0:
                    add(i, k, way, f)
            left[i, k] += sum(g == 0 for _, g in pairs)

    def fill(now):
        nonlocal count
        pool.sort()
        kept = []
        for item in pool:
            i, k, way, f = item[1]
            axis = streams[i]["order"][k]
            link = (axis, way if sizes[axis] > 2 else 0)
            if free.get(link, 0.0) - now < backlog:
                hops = f - sent_to(i, k, way, f)
                begin = max(free.get(link, 0.0), now)
                free[link] = begin + hops * message_bytes(streams[i], k, sizes) / rate
                count += 1
                heapq.heappush(events, (free[link] + latency + (hops - 1) * hop, count, item[1]))
                acts.append(("send",) + item[1])
            else:
                kept.append(item)
        pool[:] = kept

    early = [i for i, stream in enumerate(streams) if stream["order"][0] == 1]
    for i in early:
        start_stage(i, 0)
    fill(0.0)
    acts.append(("rest",))
    now = rest
    for i in range(len(streams)):
        if i not in early:
            start_stage(i, 0)
    fill(now)
    while events:
        at, _, (i, k, way, f) = heapq.heappop(events)
        now = max(now, at) + turn
        g = sent_to(i, k, way, f)
        acts.append(("recv", i, k, way, f))
        if g > 0:
            missing[i, k, way, g] -= 1
            if missing[i, k, way, g] == 0:
                acts.append(("join", i, k, way, g))
                add(i, k, way, g)
        else:
            left[i, k] -= 1
            if left[i, k] == 0:
                acts.append(("close", i, k))
                if k < 2:
                    start_stage(i, k + 1)
        fill(now)
    return acts


X, Z, Y = 0, 1, 2
PIECES = (
    (1, (1, 2, 1), (Y, X, Z), (False, False, True), -2.53),
    (0, (2, 3), (X, Y, Z), (False, True, True), 1.68),
    (0, (1, 3, 3), (Z, Y, X), (False, True, True), 2.01),
)


def make_streams(q_rows, k_rows):
    streams = [
        dict(
            peak=True,
            rows=PEAK_ROWS,
            order=(Z, X, Y),
            parity=0,
            short=(True, True, True),
            offset=0.0,
        )
    ]
    used = [0, 0]
    for kind, heights, order, short, offset in PIECES:
        for n, height in enumerate(heights):
            rows = height * (q_rows // 12, k_rows // 4)[kind]
            streams.append(
                dict(
                    peak=False,
                    kind=kind,
                    at=used[kind],
                    rows=rows,
                    order=order,
                    parity=n % 2,
                    short=short,
                    offset=offset,
                )
            )
            used[kind] += rows
    assert used == [q_rows, k_rows]
    return streams


def split(x):
    high = x.astype(jnp.bfloat16)
    low = (x - high.astype(jnp.float32)).astype(jnp.bfloat16)
    return jnp.concatenate([high, low], axis=1)


def contract_rows(a, b):
    return lax.dot_general(a, b, (((0,), (0,)), ((), ())), preferred_element_type=jnp.float32)


def gramian(pair):
    g = contract_rows(pair, pair)
    return (g[:W, :W] + g[W:, W:]) + (g[:W, W:] + g[W:, :W])


def mixer_of(gram):
    square = jnp.dot(
        gram, gram, precision=lax.Precision.HIGHEST, preferred_element_type=jnp.float32
    )
    mixer = split(COEFF_B * gram + COEFF_C * square)
    return jnp.concatenate([mixer, mixer], axis=0)


def mixed(pair, mixer):
    out = jnp.dot(pair, mixer, preferred_element_type=jnp.float32)
    return out[:, :W] + out[:, W:]


def body(
    sizes,
    q_rows,
    k_rows,
    picks,
    tokens,
    local_heads,
    streams,
    acts,
    q_lat,
    k_lat,
    q_grad_hbm,
    k_grad_hbm,
    q_heads,
    k_heads,
    q_pick,
    k_pick,
    q_weight,
    k_weight,
    q_moment,
    k_moment,
    q_weight_out,
    k_weight_out,
    q_moment_out,
    k_moment_out,
    *scratch,
):
    nx, nz, ny, nh, nc = sizes
    q_grad, k_grad, blocks, x_full, pairs, in_sem, send_sem, recv_sem = scratch[:8]
    bufs = scratch[8:]
    me = tuple(lax.axis_index(name) for name in AXES)
    rows = q_rows + k_rows

    def at(axis, shift):
        there = list(me)
        there[axis] = lax.rem(me[axis] + shift + sizes[axis], sizes[axis])
        return tuple(there)

    def nth_z(n):
        size = nz // 2 - (n + 1) // 2
        return lax.rem(me[1] + (size if n % 2 else -size) + nz, nz)

    def loop_z(n):
        size = nz // 2 - (n + 1) // 2
        return lax.rem(me[1] + jnp.where(lax.rem(n, 2) == 1, size, -size) + nz, nz)

    def reads(n, z):
        copies = []
        for x_low in range(nx // 2):
            cols = pl.ds(pl.multiple_of((x_low * nz + z) * (ny * W), ny * W), ny * W)
            for kind, (source, target) in enumerate(((q_grad_hbm, q_grad), (k_grad_hbm, k_grad))):
                copies.append(
                    pltpu.make_async_copy(
                        source.at[:, cols], target.at[:, cols], in_sem.at[n, x_low, kind]
                    )
                )
        return copies

    for n in range(nz):
        for copy in reads(n, nth_z(n)):
            copy.start()
    partners = []
    for axis in range(3):
        shifts = {nx // 2} if axis == 0 else set()
        for stream in streams:
            for way, moves in stage_routes(stream, stream["order"].index(axis), sizes).items():
                for f, g in moves:
                    shifts |= {(f - g) % sizes[axis], (g - f) % sizes[axis]}
        partners += [at(axis, s) for s in sorted(shifts) if s]
    partners += [at(3, s) for s in range(1, nh)] + [at(4, s) for s in range(1, nc)]
    barrier = pltpu.get_barrier_semaphore()
    for there in partners:
        pl.semaphore_signal(
            barrier, inc=1, device_id=there, device_id_type=pl.DeviceIdType.MESH
        )

    place = me[3] * nc + me[4]
    lane = lax.broadcasted_iota(jnp.int32, (PEAK_ROWS, W), 1)
    token = lax.broadcasted_iota(jnp.int32, (tokens, picks), 0)
    peaks = jnp.full((PEAK_ROWS, W), LOWEST, jnp.float32)
    for h in range(local_heads):
        picked = []
        for pick, heads in ((q_pick, q_heads), (k_pick, k_heads)):
            chosen = (token == pick[h]).astype(jnp.float32).astype(jnp.bfloat16)
            picked.append(contract_rows(chosen, heads[:, h * W : (h + 1) * W]))
        score = jnp.sum(picked[0] * picked[1], axis=1, keepdims=True)
        top = jnp.max(score, axis=0, keepdims=True) * SCORE_SCALE
        peaks = jnp.where(lane == place * local_heads + h, top, peaks)
    bufs[0][...] = peaks

    shaped, slot_of, sem_of, sems, pos = [], [], {}, 0, 0
    for i, stream in enumerate(streams):
        shaped.append(bufs[pos : pos + 6])
        pos += 6
        slots = {}
        for k in range(3):
            number = 0
            for way, moves in stage_routes(stream, k, sizes).items():
                for f, _ in moves:
                    slots[k, way, f] = number
                    sem_of[i, k, way, f] = sems
                    number += 1
                    sems += 1
        slot_of.append(slots)

    def terms(n, z):
        for copy in reads(n, z):
            copy.wait()
        for x_low in range(nx // 2):
            cols = pl.ds(pl.multiple_of((x_low * nz + z) * (ny * W), ny * W), ny * W)
            out = (
                jnp.dot(q_lat[...], q_grad[:, cols], preferred_element_type=jnp.float32),
                jnp.dot(k_lat[...], k_grad[:, cols], preferred_element_type=jnp.float32),
            )
            for stream, buf in zip(streams, shaped):
                if stream["peak"]:
                    continue
                for half in range(2):
                    first = half * (q_rows, k_rows)[stream["kind"]] + stream["at"]
                    for y in range(ny):
                        where = {0: half * (nx // 2) + x_low, 1: z, 2: y}
                        a, b, c = (where[axis] for axis in stream["order"])
                        buf[0][a, b, c] = out[stream["kind"]][
                            first : first + stream["rows"], y * W : (y + 1) * W
                        ]

    lead = min(3, nz)
    for n in range(lead):
        terms(n, nth_z(n))
    pl.semaphore_wait(barrier, len(partners))

    def rest_of_terms():
        group = 3 if (nz - lead) % 3 == 0 else 1

        def some(m, carry):
            for g in range(group):
                n = lead + m * group + g
                terms(n, loop_z(n))
            return carry

        lax.fori_loop(0, (nz - lead) // group, some, 0)

    def join(stream, a, b):
        return jnp.maximum(a, b) if stream["peak"] else a + b

    def own_part(i, k, which):
        stream, buf = streams[i], shaped[i]
        source = (buf[0], buf[2], buf[4])[k]
        return source if stream["peak"] else source.at[which]

    def landing(i, k):
        return (shaped[i][1], shaped[i][3], shaped[i][5])[k]

    def incoming(i, k, way, g):
        moves = stage_routes(streams[i], k, sizes).get(way, ())
        return [landing(i, k).at[slot_of[i][k, way, f]] for f, to in moves if to == g]

    def owner(i, k, way, f):
        axis = streams[i]["order"][k]
        return lax.rem(me[axis] + way * f + sizes[axis], sizes[axis])

    def remote(i, k, way, f):
        g = dict(stage_routes(streams[i], k, sizes)[way])[f]
        joined = incoming(i, k, way, f)
        source = joined[0] if joined else own_part(i, k, owner(i, k, way, f))
        sem = sem_of[i, k, way, f]
        return pltpu.make_async_remote_copy(
            src_ref=source,
            dst_ref=landing(i, k).at[slot_of[i][k, way, f]],
            send_sem=send_sem.at[sem],
            recv_sem=recv_sem.at[sem],
            device_id=at(streams[i]["order"][k], way * (f - g)),
            device_id_type=pl.DeviceIdType.MESH,
        )

    half = me[0] // (nx // 2)
    mine = blocks.at[half, me[3], me[4]]
    started = []
    for act in acts:
        if act[0] == "rest":
            rest_of_terms()
        elif act[0] == "send":
            copy = remote(*act[1:])
            copy.start()
            started.append(copy)
        elif act[0] == "recv":
            remote(*act[1:]).wait_recv()
        elif act[0] == "join":
            _, i, k, way, g = act
            landed = incoming(i, k, way, g)
            total = own_part(i, k, owner(i, k, way, g))[...]
            for part in landed:
                total = join(streams[i], total, part[...])
            landed[0][...] = total
        else:
            _, i, k = act
            stream = streams[i]
            total = own_part(i, k, me[stream["order"][k]])[...]
            for way in (-1, 1):
                for part in incoming(i, k, way, 0):
                    total = join(stream, total, part[...])
            if k < 2:
                (shaped[i][2], shaped[i][4])[k][...] = total
            elif stream["peak"]:
                mine[rows:, :] = total
            else:
                span = pl.ds(stream["at"], stream["rows"])
                moment, out = ((q_moment, q_moment_out), (k_moment, k_moment_out))[stream["kind"]]
                fresh = MOMENTUM * moment[span, :] + total
                out[span, :] = fresh
                mine[pl.ds(stream["kind"] * q_rows + stream["at"], stream["rows"]), :] = fresh

    gathered = sems
    sent = 0

    def hand_on(which, there):
        nonlocal sent
        h, y, c = which
        number = (h * nh + y) * nc + c
        copy = pltpu.make_async_remote_copy(
            src_ref=blocks.at[h, y, c],
            dst_ref=blocks.at[h, y, c],
            send_sem=send_sem.at[gathered + sent],
            recv_sem=recv_sem.at[gathered + number],
            device_id=there,
            device_id_type=pl.DeviceIdType.MESH,
        )
        copy.start()
        started.append(copy)
        sent += 1

    def arrived(which):
        h, y, c = which
        number = (h * nh + y) * nc + c
        pltpu.make_async_remote_copy(
            src_ref=blocks.at[h, y, c],
            dst_ref=blocks.at[h, y, c],
            send_sem=send_sem.at[gathered],
            recv_sem=recv_sem.at[gathered + number],
            device_id=me,
            device_id_type=pl.DeviceIdType.MESH,
        ).wait_recv()

    own = (half, me[3], me[4])
    far = (1 - half, me[3], me[4])
    hand_on(own, at(0, nx // 2))
    for s in range(1, nh):
        hand_on(own, at(3, s))
    for s in range(1, nc):
        hand_on(own, at(4, s))
    arrived(far)
    for s in range(1, nh):
        hand_on(far, at(3, s))
    for s in range(1, nc):
        hand_on(far, at(4, s))
    for h in (half, 1 - half):
        for s in range(1, nh):
            other = (h, lax.rem(me[3] - s + nh, nh), me[4])
            arrived(other)
            for s2 in range(1, nc):
                hand_on(other, at(4, s2))
    for s2 in range(1, nc):
        for h in (half, 1 - half):
            for s in range(nh):
                arrived((h, lax.rem(me[3] - s + nh, nh), lax.rem(me[4] - s2 + nc, nc)))

    head = lax.rem((me[0] * nz + me[1]) * ny + me[2], nx * nz * ny // 2)
    top = jnp.full((PEAK_ROWS, W), LOWEST, jnp.float32)
    for y in range(nh):
        for c in range(nc):
            top = jnp.maximum(top, blocks[half, y, c, rows:, :])
    top = jnp.where(lane == head, top, LOWEST)
    peak = jnp.max(jnp.max(top, axis=1, keepdims=True), axis=0, keepdims=True)
    shrink = jnp.sqrt(CLIP_LEVEL / jnp.maximum(peak, CLIP_LEVEL))

    count = 2 * nh * nc
    starts = (0, count * q_rows)
    heights = (count * q_rows, count * k_rows)
    for h in range(2):
        for y in range(nh):
            for c in range(nc):
                number = (h * nh + y) * nc + c
                block = blocks[h, y, c]
                for kind, part in ((0, block[:q_rows]), (1, block[q_rows:rows])):
                    height = (q_rows, k_rows)[kind]
                    span = pl.ds(starts[kind] + number * height, height)
                    x_full[span, :] = part
                    pairs[span, :] = split(part)

    def tile(kind):
        return pl.ds(starts[kind], heights[kind])

    eye = lax.broadcasted_iota(jnp.int32, (W, W), 0) == lax.broadcasted_iota(
        jnp.int32, (W, W), 1
    )
    mixers, scales = [], []
    for kind in range(2):
        gram = gramian(pairs[tile(kind), :])
        diagonal = jnp.where(eye, gram, 0.0)
        trace = jnp.sum(jnp.sum(diagonal, axis=1, keepdims=True), axis=0, keepdims=True)
        scale = 1.0 / jnp.sqrt(trace + 1.0)
        mixers.append(mixer_of(gram * (scale * scale)))
        scales.append(scale)
    for kind in range(2):
        fresh = scales[kind] * (
            COEFF_A * x_full[tile(kind), :] + mixed(pairs[tile(kind), :], mixers[kind])
        )
        x_full[tile(kind), :] = fresh
        pairs[tile(kind), :] = split(fresh)

    def iteration(_, carry):
        mixers = [mixer_of(gramian(pairs[tile(kind), :])) for kind in range(2)]
        for kind in range(2):
            fresh = COEFF_A * x_full[tile(kind), :] + mixed(pairs[tile(kind), :], mixers[kind])
            x_full[tile(kind), :] = fresh
            pairs[tile(kind), :] = split(fresh)
        return carry

    lax.fori_loop(0, ITERS - 2, iteration, 0)
    number = (half * nh + me[3]) * nc + me[4]
    keep = 1.0 - STEP_SIZE * DECAY
    for kind, (weight, out, rank) in enumerate(
        ((q_weight, q_weight_out, QR), (k_weight, k_weight_out, KR))
    ):
        height = (q_rows, k_rows)[kind]
        mixer = mixer_of(gramian(pairs[tile(kind), :]))
        span = pl.ds(pl.multiple_of(starts[kind] + number * height, 8), height)
        current = x_full[span, :]
        ortho = COEFF_A * current + mixed(split(current), mixer)
        out[...] = (weight[...] * keep - STEP_SIZE * 0.2 * math.sqrt(rank) * ortho) * shrink
    for copy in started:
        copy.wait_send()


def step(sizes, q_rows, k_rows, picks, tokens, local_heads):
    streams = make_streams(q_rows, k_rows)
    acts = plan(streams, sizes)
    rows = q_rows + k_rows
    width = sizes[0] * sizes[1] * sizes[2] // 2 * W
    count = 2 * sizes[3] * sizes[4]
    scratch = [
        pltpu.VMEM((tokens, width), jnp.bfloat16),
        pltpu.VMEM((tokens, width), jnp.bfloat16),
        pltpu.VMEM((2, sizes[3], sizes[4], rows + PEAK_ROWS, W), jnp.float32),
        pltpu.VMEM((count * rows, W), jnp.float32),
        pltpu.VMEM((count * rows, 2 * W), jnp.bfloat16),
        pltpu.SemaphoreType.DMA((sizes[1], sizes[0] // 2, 2)),
    ]
    messages = 0
    bufs = []
    for stream in streams:
        n = [sizes[axis] for axis in stream["order"]]
        messages += sum(n) - 3
        tile = (stream["rows"], W)
        lead = [(), (), ()] if stream["peak"] else [(n[1], n[2]), (n[2],), ()]
        for k in range(3):
            source = lead[k] if stream["peak"] else (n[k],) + lead[k]
            bufs.append(pltpu.VMEM(source + tile, jnp.float32))
            bufs.append(pltpu.VMEM((max(n[k] - 1, 1),) + lead[k] + tile, jnp.float32))
    scratch += [
        pltpu.SemaphoreType.DMA((messages + count,)),
        pltpu.SemaphoreType.DMA((messages + count,)),
    ]
    vmem = pl.BlockSpec(memory_space=pltpu.VMEM)
    hbm = pl.BlockSpec(memory_space=pltpu.HBM)
    return pl.pallas_call(
        functools.partial(
            body, sizes, q_rows, k_rows, picks, tokens, local_heads, streams, acts
        ),
        out_shape=[
            pltpu.VMEM((q_rows, W), jnp.float32),
            pltpu.VMEM((k_rows, W), jnp.float32),
            pltpu.VMEM((q_rows, W), jnp.float32),
            pltpu.VMEM((k_rows, W), jnp.float32),
        ],
        in_specs=[vmem, vmem, hbm, hbm] + [vmem] * 8,
        out_specs=[vmem] * 4,
        scratch_shapes=scratch + bufs,
        compiler_params=pltpu.CompilerParams(
            collective_id=0, has_side_effects=True, vmem_limit_bytes=60 * 1024 * 1024
        ),
        name="muon_clip",
    )


def hand_out(*refs):
    for source, target in zip(refs[:4], refs[4:]):
        target[...] = source[...]


def handed_out(arrays):
    vmem = pl.BlockSpec(memory_space=pltpu.VMEM)
    return pl.pallas_call(
        hand_out,
        out_shape=[jax.ShapeDtypeStruct(a.shape, a.dtype) for a in arrays],
        in_specs=[vmem] * 4,
        out_specs=[vmem] * 4,
        compiler_params=pltpu.CompilerParams(vmem_limit_bytes=2 * 1024 * 1024),
        name="hand_out",
    )(*arrays)


def local(
    sizes,
    q_latent,
    kv_latent,
    q_head_grad,
    k_head_grad,
    q_heads,
    k_heads,
    query_pick,
    key_pick,
    q_weight,
    k_weight,
    q_moment,
    k_moment,
):
    tokens, _, q_rows = q_latent.shape
    k_rows = kv_latent.shape[2]
    picks, local_heads = query_pick.shape[1:]
    out = step(sizes, q_rows, k_rows, picks, tokens, local_heads)(
        q_latent.transpose(1, 2, 0).reshape(2 * q_rows, tokens),
        kv_latent.transpose(1, 2, 0).reshape(2 * k_rows, tokens),
        q_head_grad,
        k_head_grad,
        q_heads,
        k_heads,
        query_pick.transpose(2, 0, 1),
        key_pick.transpose(2, 0, 1),
        q_weight[0],
        k_weight[0],
        q_moment[0],
        k_moment[0],
    )
    return tuple(array[None] for array in handed_out(out))


def solution(mesh, sizes=SHAPE):
    axes = Mesh(mesh.devices.reshape(sizes), AXES)
    placed = (
        P(DP, None, MP),
        P(DP, None, MP),
        P(DP, None),
        P(DP, None),
        P(DP, MP),
        P(DP, MP),
        P(DP, None, MP),
        P(DP, None, MP),
        P(DP, MP, None),
        P(DP, MP, None),
        P(DP, MP, None),
        P(DP, MP, None),
    )
    return jax.shard_map(
        functools.partial(local, sizes),
        mesh=axes,
        in_specs=placed,
        out_specs=(P(DP, MP, None),) * 4,
        check_vma=False,
    )
```

```python
import functools
import heapq
import math

import jax
import jax.numpy as jnp
from jax import lax
from jax.experimental import pallas as pl
from jax.experimental.pallas import tpu as pltpu
from jax.sharding import Mesh
from jax.sharding import PartitionSpec as P

QR = 1536
KR = 512
ITERS = 5
AXES = ("dp_0", "dp_1", "dp_2", "mp_0", "mp_1")
DP = AXES[:3]
MP = AXES[3:]
SHAPE = (4, 12, 2, 4, 2)

MOMENTUM = 0.95
STEP_SIZE = 1.0
DECAY = 0.1
CLIP_LEVEL = 0.1
SCORE_SCALE = 1.0 / math.sqrt(192.0)
COEFF_A = 3.4445
COEFF_B = -4.775
COEFF_C = 2.0315
LOWEST = -1e30
W = 128
PEAK_ROWS = 8


SHORT = {
    1: ((1, 0),),
    2: ((2, 0), (1, 0)),
    3: ((1, 0), (3, 2), (2, 0)),
    5: ((1, 0), (3, 2), (5, 4), (4, 2), (2, 0)),
    6: ((1, 0), (3, 2), (5, 4), (6, 4), (4, 2), (2, 0)),
}
FLAT = {
    **SHORT,
    5: ((3, 2), (1, 2), (5, 4), (4, 0), (2, 0)),
    6: ((3, 2), (1, 2), (6, 5), (4, 5), (5, 0), (2, 0)),
}


def routes(n, parity, form):
    far, near = n // 2, n - 1 - n // 2
    lengths = {-1: far, 1: near} if parity == 0 else {-1: near, 1: far}
    found = {}
    for way, length in lengths.items():
        if length:
            chain = tuple((f, f - 1) for f in range(length, 0, -1))
            found[way] = ({}, SHORT, FLAT)[form].get(length, chain)
    return found


def stage_routes(stream, stage, sizes):
    return routes(sizes[stream["order"][stage]], stream["parity"], stream["forms"][stage])


def message_bytes(stream, stage, sizes):
    size = stream["rows"] * W * 4
    if not stream["peak"]:
        for axis in stream["order"][stage + 1 :]:
            size *= sizes[axis]
    return size


def plan(
    streams, groups, sizes, rate=47.5e3, latency=2.5, hop=0.75, backlog=5.0, turn=0.12, rest=3.5
):
    free, pool, acts, events, left, missing = {}, [], [], [], {}, {}
    count = 0
    ways = [[stage_routes(stream, k, sizes) for k in range(3)] for stream in streams]
    unfinished = [len(members) for members in groups]
    group_of = {i: g for g, members in enumerate(groups) for i in members}
    group_bytes = [sum(streams[i]["rows"] for i in members) * W * 4 for members in groups]
    shifts = sorted(range(1, sizes[3]), key=lambda s: abs(2 * s - sizes[3]))

    def sent_to(i, k, way, f):
        return dict(ways[i][k][way])[f]

    def lasts(i, k, way, f):
        time = 0.0
        while f > 0:
            g = sent_to(i, k, way, f)
            time += latency + turn + (f - g - 1) * hop
            time += (f - g) * message_bytes(streams[i], k, sizes) / rate
            f = g
        return time

    def add(i, k, way, f):
        time = lasts(i, k, way, f) + 9.0
        for later in range(k + 1, 3):
            time += max(
                lasts(i, later, w, start) for w, pairs in ways[i][later].items() for start, _ in pairs
            )
        pool.append((i - time + streams[i]["offset"], ("sum", i, k, way, f)))

    def start_stage(i, k):
        left[i, k] = 0
        for way, pairs in ways[i][k].items():
            for f, _ in pairs:
                missing[i, k, way, f] = sum(g == f for _, g in pairs)
                if missing[i, k, way, f] == 0:
                    add(i, k, way, f)
            left[i, k] += sum(g == 0 for _, g in pairs)

    def load(message):
        if message[0] == "sum":
            _, i, k, way, f = message
            axis = streams[i]["order"][k]
            hops = f - sent_to(i, k, way, f)
            size = hops * message_bytes(streams[i], k, sizes)
            both = (("y", 1), ("y", -1))
            return [(link, size) for link in (both if axis == 2 else ((axis, way),))], hops
        size = group_bytes[message[1]]
        if message[0] == "across":
            return [((0, 1), size), ((0, -1), size)], 2
        s, half = 2 * message[2], sizes[3]
        taken = [((0, 1), size), ((0, -1), size)] if message[0] == "cross" else []
        hops = 2 if message[0] == "cross" else 0
        if s == half:
            return taken + [(("y", 1), 2 * size), (("y", -1), 2 * size)], hops + 4
        return taken + [(("y", 1 if s < half else -1), 2 * size)], hops + 2

    def fill(now):
        nonlocal count
        pool.sort()
        kept = []
        for item in pool:
            taken, hops = load(item[1])
            if max(free.get(link, 0.0) for link, _ in taken) - now < backlog:
                end = 0.0
                for link, size in taken:
                    free[link] = max(free.get(link, 0.0), now) + size / rate
                    end = max(end, free[link])
                count += 1
                heapq.heappush(events, (end + latency + (hops - 1) * hop, count, item[1]))
                acts.append(("send", item[1]))
            else:
                kept.append(item)
        pool[:] = kept

    early = [i for i, stream in enumerate(streams) if stream["order"][0] == 1]
    assert 0 not in early
    for i in early:
        start_stage(i, 0)
    fill(0.0)
    acts.append(("rest",))
    now = rest
    for i in range(len(streams)):
        if i not in early:
            start_stage(i, 0)
    fill(now)
    while events:
        at, _, message = heapq.heappop(events)
        now = max(now, at) + turn
        acts.append(("recv", message))
        if message[0] == "sum":
            _, i, k, way, f = message
            g = sent_to(i, k, way, f)
            if g > 0:
                missing[i, k, way, g] -= 1
                if missing[i, k, way, g] == 0:
                    acts.append(("join", i, k, way, g))
                    add(i, k, way, g)
            else:
                left[i, k] -= 1
                if left[i, k] == 0:
                    acts.append(("close", i, k))
                    if k < 2:
                        start_stage(i, k + 1)
                    else:
                        ready = group_of[i]
                        unfinished[ready] -= 1
                        if unfinished[ready] == 0:
                            acts.append(("ready", ready))
                            pool.append((-31.0, ("across", ready)))
                            for n, s in enumerate(shifts):
                                pool.append((-21.0 + min(n, 1), ("own", ready, s)))
                                if ready not in RELAYED:
                                    pool.append((-16.0 + min(n, 1), ("cross", ready, s)))
        elif message[0] == "across" and message[1] in RELAYED:
            for n, s in enumerate(shifts):
                pool.append((-11.0 + min(n, 1), ("far", message[1], s)))
        fill(now)
    return acts


X, Z, Y = 0, 1, 2
PIECES = (
    (1, (1, 2, 1), (Y, X, Z), (0, 0, 1), -2.53),
    (0, (2, 3), (X, Y, Z), (0, 1, 1), 1.68),
    (0, (1, 3, 3), (Z, Y, X), (0, 1, 1), 2.01),
)
GROUPS = ((4, 5), (6, 7, 8), (1, 2, 3, 0))
RELAYED = (0, 1, 2)


def make_streams(q_rows, k_rows):
    streams = [
        dict(
            peak=True,
            rows=PEAK_ROWS,
            order=(X, Y, Z),
            parity=0,
            forms=(1, 1, 1),
            offset=0.0,
        )
    ]
    used = [0, 0]
    for kind, heights, order, forms, offset in PIECES:
        for n, height in enumerate(heights):
            rows = height * (q_rows // 12, k_rows // 4)[kind]
            streams.append(
                dict(
                    peak=False,
                    kind=kind,
                    at=used[kind],
                    rows=rows,
                    order=order,
                    parity=n % 2,
                    forms=forms,
                    offset=offset,
                )
            )
            used[kind] += rows
    assert used == [q_rows, k_rows]
    return streams


def split(x):
    high = x.astype(jnp.bfloat16)
    low = (x - high.astype(jnp.float32)).astype(jnp.bfloat16)
    return jnp.concatenate([high, low], axis=1)


def contract_rows(a, b):
    return lax.dot_general(a, b, (((0,), (0,)), ((), ())), preferred_element_type=jnp.float32)


def gramian(pair):
    return folded(contract_rows(pair, pair))


def folded(g):
    return (g[:W, :W] + g[W:, W:]) + (g[:W, W:] + g[W:, :W])


def mixer_of(gram):
    pair = split(gram)
    square = mixed(pair, jnp.concatenate([pair, pair], axis=0))
    mixer = split(COEFF_B * gram + COEFF_C * square)
    return jnp.concatenate([mixer, mixer], axis=0)


def mixed(pair, mixer):
    out = jnp.dot(pair, mixer, preferred_element_type=jnp.float32)
    return out[:, :W] + out[:, W:]


def body(
    sizes,
    q_rows,
    k_rows,
    picks,
    tokens,
    local_heads,
    streams,
    acts,
    q_lat,
    k_lat,
    q_grad_hbm,
    k_grad_hbm,
    q_heads,
    k_heads,
    q_pick,
    k_pick,
    q_weight,
    k_weight,
    q_moment,
    k_moment,
    q_weight_out,
    k_weight_out,
    q_moment_out,
    k_moment_out,
    *scratch,
):
    nx, nz, ny, nh, nc = sizes
    q_grad, k_grad, blocks, x_full, pairs, in_sem, send_sem, recv_sem = scratch[:8]
    bufs = scratch[8:]
    me = tuple(lax.axis_index(name) for name in AXES)
    rows = q_rows + k_rows

    def at(axis, shift, origin=me):
        there = list(origin)
        there[axis] = lax.rem(me[axis] + shift + sizes[axis], sizes[axis])
        return tuple(there)

    def nth_z(n):
        size = nz // 2 - (n + 1) // 2
        return lax.rem(me[1] + (size if n % 2 else -size) + nz, nz)

    def loop_z(n):
        size = nz // 2 - (n + 1) // 2
        return lax.rem(me[1] + jnp.where(lax.rem(n, 2) == 1, size, -size) + nz, nz)

    def reads(n, z):
        copies = []
        for x_low in range(nx // 2):
            cols = pl.ds(pl.multiple_of((x_low * nz + z) * (ny * W), ny * W), ny * W)
            for kind, (source, target) in enumerate(((q_grad_hbm, q_grad), (k_grad_hbm, k_grad))):
                copies.append(
                    pltpu.make_async_copy(
                        source.at[:, cols], target.at[:, cols], in_sem.at[n, x_low, kind]
                    )
                )
        return copies

    for n in range(nz):
        for copy in reads(n, nth_z(n)):
            copy.start()
    partners = []
    for axis in range(3):
        shifts = {nx // 2} if axis == 0 else set()
        for stream in streams:
            for way, moves in stage_routes(stream, stream["order"].index(axis), sizes).items():
                for f, g in moves:
                    shifts |= {(f - g) % sizes[axis], (g - f) % sizes[axis]}
        partners += [at(axis, s) for s in sorted(shifts) if s]
    opposite = at(0, nx // 2)
    partners += [at(3, s) for s in range(1, nh)] + [at(4, s) for s in range(1, nc)]
    partners += [at(3, s, opposite) for s in range(1, nh)]
    barrier = pltpu.get_barrier_semaphore()
    for there in partners:
        pl.semaphore_signal(
            barrier, inc=1, device_id=there, device_id_type=pl.DeviceIdType.MESH
        )


    shaped, slot_of, sem_of, sems, pos = [], [], {}, 0, 0
    for i, stream in enumerate(streams):
        shaped.append(bufs[pos : pos + 6])
        pos += 6
        slots = {}
        for k in range(3):
            number = 0
            for way, moves in stage_routes(stream, k, sizes).items():
                for f, _ in moves:
                    slots[k, way, f] = number
                    sem_of[i, k, way, f] = sems
                    number += 1
                    sems += 1
        slot_of.append(slots)

    def terms(n, z):
        for copy in reads(n, z):
            copy.wait()
        for x_low in range(nx // 2):
            cols = pl.ds(pl.multiple_of((x_low * nz + z) * (ny * W), ny * W), ny * W)
            out = (
                jnp.dot(q_lat[...], q_grad[:, cols], preferred_element_type=jnp.float32),
                jnp.dot(k_lat[...], k_grad[:, cols], preferred_element_type=jnp.float32),
            )
            for stream, buf in zip(streams, shaped):
                if stream["peak"]:
                    continue
                for half in range(2):
                    first = half * (q_rows, k_rows)[stream["kind"]] + stream["at"]
                    for y in range(ny):
                        where = {0: half * (nx // 2) + x_low, 1: z, 2: y}
                        a, b, c = (where[axis] for axis in stream["order"])
                        buf[0][a, b, c] = out[stream["kind"]][
                            first : first + stream["rows"], y * W : (y + 1) * W
                        ]

    lead = min(3, nz)
    for n in range(lead):
        terms(n, nth_z(n))
    pl.semaphore_wait(barrier, len(partners))

    lane = lax.broadcasted_iota(jnp.int32, (PEAK_ROWS, W), 1)

    def scores():
        place = me[3] * nc + me[4]
        token = lax.broadcasted_iota(jnp.int32, (tokens, picks), 0)
        peaks = jnp.full((PEAK_ROWS, W), LOWEST, jnp.float32)
        for h in range(local_heads):
            picked = []
            for pick, heads in ((q_pick, q_heads), (k_pick, k_heads)):
                chosen = (token == pick[h]).astype(jnp.float32).astype(jnp.bfloat16)
                picked.append(contract_rows(chosen, heads[:, h * W : (h + 1) * W]))
            score = jnp.sum(picked[0] * picked[1], axis=1, keepdims=True)
            top = jnp.max(score, axis=0, keepdims=True) * SCORE_SCALE
            peaks = jnp.where(lane == place * local_heads + h, top, peaks)
        bufs[0][...] = peaks

    def rest_of_terms():
        group = 3 if (nz - lead) % 3 == 0 else 1

        def some(m, carry):
            for g in range(group):
                n = lead + m * group + g
                terms(n, loop_z(n))
            return carry

        lax.fori_loop(0, (nz - lead) // group, some, 0)

    def join(stream, a, b):
        return jnp.maximum(a, b) if stream["peak"] else a + b

    def own_part(i, k, which):
        stream, buf = streams[i], shaped[i]
        source = (buf[0], buf[2], buf[4])[k]
        return source if stream["peak"] else source.at[which]

    def landing(i, k):
        return (shaped[i][1], shaped[i][3], shaped[i][5])[k]

    def incoming(i, k, way, g):
        moves = stage_routes(streams[i], k, sizes).get(way, ())
        return [landing(i, k).at[slot_of[i][k, way, f]] for f, to in moves if to == g]

    def owner(i, k, way, f):
        axis = streams[i]["order"][k]
        return lax.rem(me[axis] + way * f + sizes[axis], sizes[axis])

    def remote(i, k, way, f):
        g = dict(stage_routes(streams[i], k, sizes)[way])[f]
        joined = incoming(i, k, way, f)
        source = joined[0] if joined else own_part(i, k, owner(i, k, way, f))
        sem = sem_of[i, k, way, f]
        return pltpu.make_async_remote_copy(
            src_ref=source,
            dst_ref=landing(i, k).at[slot_of[i][k, way, f]],
            send_sem=send_sem.at[sem],
            recv_sem=recv_sem.at[sem],
            device_id=at(streams[i]["order"][k], way * (f - g)),
            device_id_type=pl.DeviceIdType.MESH,
        )

    half = me[0] // (nx // 2)
    mine = blocks.at[half, me[3], me[4]]
    spans = []
    for members in GROUPS:
        height = sum(streams[i]["rows"] for i in members)
        spans.append((sum(n for _, n in spans), height))
    gathered = sems
    sent = 0

    def gather_copy(h, y, c, g, there, send):
        number = ((h * nh + y) * nc + c) * len(GROUPS) + g
        part = blocks.at[h, y, c, pl.ds(*spans[g])]
        return pltpu.make_async_remote_copy(
            src_ref=part,
            dst_ref=part,
            send_sem=send_sem.at[gathered + send],
            recv_sem=recv_sem.at[gathered + number],
            device_id=there,
            device_id_type=pl.DeviceIdType.MESH,
        )

    def hand_on(h, y, c, g, there):
        nonlocal sent
        copy = gather_copy(h, y, c, g, there, sent)
        copy.start()
        started.append(copy)
        sent += 1

    def to_other_cores(h, y, g):
        for s in range(1, nc):
            hand_on(h, y, me[4], g, at(4, s))

    def arrived(h, y, c, g):
        gather_copy(h, y, c, g, me, 0).wait_recv()

    def send(message):
        if message[0] == "sum":
            copy = remote(*message[1:])
            copy.start()
            started.append(copy)
        elif message[0] == "across":
            hand_on(half, me[3], me[4], message[1], opposite)
        elif message[0] == "cross":
            hand_on(half, me[3], me[4], message[1], at(3, message[2], opposite))
        else:
            hand_on(
                half if message[0] == "own" else 1 - half,
                me[3],
                me[4],
                message[1],
                at(3, message[2]),
            )

    def receive(message):
        if message[0] == "sum":
            remote(*message[1:]).wait_recv()
            return
        g = message[1]
        if message[0] == "across":
            h, y = 1 - half, me[3]
        else:
            h = half if message[0] == "own" else 1 - half
            y = lax.rem(me[3] - message[2] + nh, nh)
        arrived(h, y, me[4], g)
        to_other_cores(h, y, g)

    started = []
    for act in acts:
        if act[0] == "rest":
            scores()
            rest_of_terms()
        elif act[0] == "send":
            send(act[1])
        elif act[0] == "recv":
            receive(act[1])
        elif act[0] == "ready":
            to_other_cores(half, me[3], act[1])
        elif act[0] == "join":
            _, i, k, way, g = act
            landed = incoming(i, k, way, g)
            total = own_part(i, k, owner(i, k, way, g))[...]
            for part in landed:
                total = join(streams[i], total, part[...])
            landed[0][...] = total
        else:
            _, i, k = act
            stream = streams[i]
            total = own_part(i, k, me[stream["order"][k]])[...]
            for way in (-1, 1):
                for part in incoming(i, k, way, 0):
                    total = join(stream, total, part[...])
            if k < 2:
                (shaped[i][2], shaped[i][4])[k][...] = total
            elif stream["peak"]:
                mine[rows:, :] = total
            else:
                span = pl.ds(stream["at"], stream["rows"])
                moment, out = ((q_moment, q_moment_out), (k_moment, k_moment_out))[stream["kind"]]
                fresh = MOMENTUM * moment[span, :] + total
                out[span, :] = fresh
                mine[pl.ds(stream["kind"] * q_rows + stream["at"], stream["rows"]), :] = fresh

    count = 2 * nh * nc
    eye = lax.broadcasted_iota(jnp.int32, (W, W), 0) == lax.broadcasted_iota(
        jnp.int32, (W, W), 1
    )
    starts, grams = [], [None, None]
    for g, (first, height) in enumerate(spans):
        for s in range(1, nc):
            for h in (half, 1 - half):
                for t in range(nh):
                    other = lax.rem(me[4] - s + nc, nc)
                    arrived(h, lax.rem(me[3] - t + nh, nh), other, g)
        kind = 0 if first < q_rows else 1
        height = min(height, rows - first)
        starts.append((kind, count * first, height))
        for h in range(2):
            for y in range(nh):
                for c in range(nc):
                    number = (h * nh + y) * nc + c
                    part = blocks[h, y, c, first : first + height, :]
                    span = pl.ds(count * first + number * height, height)
                    x_full[span, :] = part
                    pairs[span, :] = split(part)
        share = pairs[count * first : count * (first + height), :]
        share = contract_rows(share, share)
        grams[kind] = share if grams[kind] is None else grams[kind] + share

    head = lax.rem((me[0] * nz + me[1]) * ny + me[2], nx * nz * ny // 2)
    top = jnp.full((PEAK_ROWS, W), LOWEST, jnp.float32)
    for y in range(nh):
        for c in range(nc):
            top = jnp.maximum(top, blocks[half, y, c, rows:, :])
    top = jnp.where(lane == head, top, LOWEST)
    peak = jnp.max(jnp.max(top, axis=1, keepdims=True), axis=0, keepdims=True)
    shrink = jnp.sqrt(CLIP_LEVEL / jnp.maximum(peak, CLIP_LEVEL))

    bounds = ((0, count * q_rows), (count * q_rows, count * k_rows))

    def tile(kind):
        return pl.ds(*bounds[kind])

    mixers, scales = [], []
    for kind in range(2):
        gram = folded(grams[kind])
        diagonal = jnp.where(eye, gram, 0.0)
        trace = jnp.sum(jnp.sum(diagonal, axis=1, keepdims=True), axis=0, keepdims=True)
        scale = 1.0 / jnp.sqrt(trace + 1.0)
        mixers.append(mixer_of(gram * (scale * scale)))
        scales.append(scale)
    for kind in range(2):
        fresh = scales[kind] * (
            COEFF_A * x_full[tile(kind), :] + mixed(pairs[tile(kind), :], mixers[kind])
        )
        x_full[tile(kind), :] = fresh
        pairs[tile(kind), :] = split(fresh)

    def iteration(_, carry):
        mixers = [mixer_of(gramian(pairs[tile(kind), :])) for kind in range(2)]
        for kind in range(2):
            fresh = COEFF_A * x_full[tile(kind), :] + mixed(pairs[tile(kind), :], mixers[kind])
            x_full[tile(kind), :] = fresh
            pairs[tile(kind), :] = split(fresh)
        return carry

    lax.fori_loop(0, ITERS - 2, iteration, 0)
    number = (half * nh + me[3]) * nc + me[4]
    keep = 1.0 - STEP_SIZE * DECAY
    for kind, (weight, out, rank) in enumerate(
        ((q_weight, q_weight_out, QR), (k_weight, k_weight_out, KR))
    ):
        mixer = mixer_of(gramian(pairs[tile(kind), :]))
        current = jnp.concatenate(
            [
                x_full[pl.ds(pl.multiple_of(at_row + number * n, 8), n), :]
                for which, at_row, n in starts
                if which == kind
            ],
            axis=0,
        )
        ortho = COEFF_A * current + mixed(split(current), mixer)
        out[...] = (weight[...] * keep - STEP_SIZE * 0.2 * math.sqrt(rank) * ortho) * shrink
    for copy in started:
        copy.wait_send()


def step(sizes, q_rows, k_rows, picks, tokens, local_heads):
    streams = make_streams(q_rows, k_rows)
    acts = plan(streams, GROUPS, sizes)
    rows = q_rows + k_rows
    width = sizes[0] * sizes[1] * sizes[2] // 2 * W
    count = 2 * sizes[3] * sizes[4]
    scratch = [
        pltpu.VMEM((tokens, width), jnp.bfloat16),
        pltpu.VMEM((tokens, width), jnp.bfloat16),
        pltpu.VMEM((2, sizes[3], sizes[4], rows + PEAK_ROWS, W), jnp.float32),
        pltpu.VMEM((count * rows, W), jnp.float32),
        pltpu.VMEM((count * rows, 2 * W), jnp.bfloat16),
        pltpu.SemaphoreType.DMA((sizes[1], sizes[0] // 2, 2)),
    ]
    messages = 0
    bufs = []
    for stream in streams:
        n = [sizes[axis] for axis in stream["order"]]
        messages += sum(n) - 3
        tile = (stream["rows"], W)
        lead = [(), (), ()] if stream["peak"] else [(n[1], n[2]), (n[2],), ()]
        for k in range(3):
            source = lead[k] if stream["peak"] else (n[k],) + lead[k]
            bufs.append(pltpu.VMEM(source + tile, jnp.float32))
            bufs.append(pltpu.VMEM((max(n[k] - 1, 1),) + lead[k] + tile, jnp.float32))
    scratch += [
        pltpu.SemaphoreType.DMA((messages + count * len(GROUPS),)),
        pltpu.SemaphoreType.DMA((messages + count * len(GROUPS),)),
    ]
    vmem = pl.BlockSpec(memory_space=pltpu.VMEM)
    hbm = pl.BlockSpec(memory_space=pltpu.HBM)
    return pl.pallas_call(
        functools.partial(
            body, sizes, q_rows, k_rows, picks, tokens, local_heads, streams, acts
        ),
        out_shape=[
            pltpu.VMEM((q_rows, W), jnp.float32),
            pltpu.VMEM((k_rows, W), jnp.float32),
            pltpu.VMEM((q_rows, W), jnp.float32),
            pltpu.VMEM((k_rows, W), jnp.float32),
        ],
        in_specs=[vmem, vmem, hbm, hbm] + [vmem] * 8,
        out_specs=[vmem] * 4,
        scratch_shapes=scratch + bufs,
        compiler_params=pltpu.CompilerParams(
            collective_id=0, has_side_effects=True, vmem_limit_bytes=60 * 1024 * 1024
        ),
        name="muon_clip",
    )


def hand_out(*refs):
    for source, target in zip(refs[:4], refs[4:]):
        target[...] = source[...]


def handed_out(arrays):
    vmem = pl.BlockSpec(memory_space=pltpu.VMEM)
    return pl.pallas_call(
        hand_out,
        out_shape=[jax.ShapeDtypeStruct(a.shape, a.dtype) for a in arrays],
        in_specs=[vmem] * 4,
        out_specs=[vmem] * 4,
        compiler_params=pltpu.CompilerParams(vmem_limit_bytes=2 * 1024 * 1024),
        name="hand_out",
    )(*arrays)


def local(
    sizes,
    q_latent,
    kv_latent,
    q_head_grad,
    k_head_grad,
    q_heads,
    k_heads,
    query_pick,
    key_pick,
    q_weight,
    k_weight,
    q_moment,
    k_moment,
):
    tokens, _, q_rows = q_latent.shape
    k_rows = kv_latent.shape[2]
    picks, local_heads = query_pick.shape[1:]
    out = step(sizes, q_rows, k_rows, picks, tokens, local_heads)(
        q_latent.transpose(1, 2, 0).reshape(2 * q_rows, tokens),
        kv_latent.transpose(1, 2, 0).reshape(2 * k_rows, tokens),
        q_head_grad,
        k_head_grad,
        q_heads,
        k_heads,
        query_pick.transpose(2, 0, 1),
        key_pick.transpose(2, 0, 1),
        q_weight[0],
        k_weight[0],
        q_moment[0],
        k_moment[0],
    )
    return tuple(array[None] for array in handed_out(out))


def solution(mesh, sizes=SHAPE):
    axes = Mesh(mesh.devices.reshape(sizes), AXES)
    placed = (
        P(DP, None, MP),
        P(DP, None, MP),
        P(DP, None),
        P(DP, None),
        P(DP, MP),
        P(DP, MP),
        P(DP, None, MP),
        P(DP, None, MP),
        P(DP, MP, None),
        P(DP, MP, None),
        P(DP, MP, None),
        P(DP, MP, None),
    )
    return jax.shard_map(
        functools.partial(local, sizes),
        mesh=axes,
        in_specs=placed,
        out_specs=(P(DP, MP, None),) * 4,
        check_vma=False,
    )
```
